256 devices in a mesh: dp: 32 (over x, z), tp: 8 (over y, core).
Axes of the slice: x: 4, y: 4, z: 8, core: 2. Of those that a mesh axis runs over, the one named last changes fastest.
Arguments:
- hidden_state: bfloat16 [7168, 512], P(None, 'dp'), may hold values from -6 to 6
- attention_gain: float32 [7168], replicated, may hold values from 0.1 to 1.9
- down_weight: bfloat16 [7168, 2112], P(None, 'tp'), may hold values from -0.0625 to 0.0625
- query_gain: float32 [1536], replicated, may hold values from 0.1 to 1.9
- latent_gain: float32 [512], replicated, may hold values from 0.1 to 1.9
- query_weight: bfloat16 [128, 576, 1536], P('tp', 'dp'), may hold values from -0.15625 to 0.15625
- latent_cache: bfloat16 [256, 4096, 576], P('dp'), may hold values from -240 to 240
- cache_length: int32 [256], P('dp'), may hold values from 1 to 4096
- owner_place: int32 [256], replicated, may hold values from 0 to 255, each once
- accept_length: int32 [256], replicated, may hold values from 1 to 2
- value_weight: bfloat16 [128, 512, 128], P('tp'), may hold values from -0.25 to 0.25
- output_weight: bfloat16 [7168, 16384], P('dp', 'tp'), may hold values from -0.046875 to 0.046875
- final_gain: float32 [7168], replicated, may hold values from 0.1 to 1.9
- head_weight: bfloat16 [7168, 65536], P(None, ('dp', 'tp')), may hold values from -8 to 8
- draft_tokens: int32 [256, 2], replicated, may hold values from 0 to 65535
Outputs:
- log_probs: float32 [512, 65536], P(None, ('dp', 'tp'))
- draft_scores: float32 [512], replicated
- committed: bfloat16 [256, 2, 576], P('dp')
The draws below stay inside these ranges and needn't reach their ends.
All inputs are finite; a program needn't handle non-finite values.
Results may differ from the reference program's by a relative error of at most 0.006.
The reference program's roundings to bfloat16 on the way count: a program that leaves them out, or rounds other values in their place, can miss the bound.
Values may be sent and summed in bfloat16 or wider, within the bound.
No kernel may reach another device: no remote copies, remote signals or barrier semaphores. Data moves between devices by JAX's collectives and lax.ppermute only.
A program may use at most 192 MiB of HBM per device.

```python
import math
import jax
import jax.numpy as jnp
import numpy as np
from jax import lax

D = 7168
QL = 1536
DL = 512
DR = 64
H = 128
HV = 128
STEPS = 2
CTX = 4096
DC = 576
VOCAB = 65536
REQS = 256
ROWS = 512


def draw_latent_cache(key, part):
    sample = jax.random.normal(key, (REQS, CTX, DL + DR), jnp.float32)
    return jnp.clip(sample, -240.0, 240.0).astype(jnp.bfloat16)


def draw_head_weight(key, part):
    sample = jax.random.normal(key, (D, VOCAB), jnp.float32) * (4.0 / math.sqrt(D))
    return jnp.clip(sample, -8.0, 8.0).astype(jnp.bfloat16)


def with_ends(entries, stream_key, smallest, largest):
    shape = entries.shape
    place = [jax.random.randint(jax.random.fold_in(stream_key, axis), (), 0, shape[axis]) for axis in range(len(shape))]
    entries = entries.at[tuple(place)].set(smallest)
    longest = shape.index(max(shape))
    place[longest] = (place[longest] + 1) % shape[longest]
    return entries.at[tuple(place)].set(largest)


def level_of(key, extent, shards, smallest, high):
    level = 1.0
    for dim, shards_of in shards:
        draws = jax.random.uniform(jax.random.fold_in(jax.random.fold_in(key, 6), dim), (shards_of,), jnp.float32, smallest / len(shards), high / len(shards))
        level = level * jnp.repeat(jnp.exp(draws), extent[dim] // shards_of).reshape((-1,) + (1,) * (len(extent) - 1 - dim))
    return level


def rank_bounds(count, skew):
    portions = [(1 << 20) // math.isqrt(grade ** skew) + 1 for grade in range(1, count + 1)]
    width = 1 + sum(portions) // (1 << 30)
    return np.cumsum(np.array([max(1, weight // width) for weight in portions]))


def ranked_ids(key, shape, number_of, skew):
    grid = rank_bounds(number_of, skew)
    pick = jax.random.randint(jax.random.fold_in(key, 1), shape, 0, int(grid[number_of - 1]))
    rank = jnp.searchsorted(jnp.asarray(grid, jnp.int32), pick, side="right")
    return jax.random.permutation(jax.random.fold_in(key, 2), number_of)[rank].astype(jnp.int32)


def scatter_about(stream_key, extent, spread, bound, shards=(), kind=jnp.bfloat16):
    level = level_of(stream_key, extent, shards, -0.22, 0.18) if shards else 1.0
    drawn = jax.random.normal(stream_key, extent, jnp.float32) * spread * level
    return jnp.minimum(jnp.maximum(drawn, -bound), bound).astype(kind)


def setup_inputs(seed: int = 0) -> dict:
    seeds = jax.random.split(jax.random.key(seed), 16)
    hidden_state = scatter_about(seeds[0], (D, ROWS), 1.0, 6.0, ((1, 32),))
    attention_gain = jnp.clip(1.0 + 0.18 * jax.random.normal(seeds[1], (D,), jnp.float32), 0.1, 1.9)
    down_weight = scatter_about(seeds[2], (D, QL + DC), D ** -0.5, 0.0625, ((1, 8),))
    query_gain = jnp.clip(1.0 + 0.18 * jax.random.normal(seeds[3], (QL,), jnp.float32), 0.1, 1.9)
    latent_gain = jnp.clip(1.0 + 0.18 * jax.random.normal(seeds[4], (DL,), jnp.float32), 0.1, 1.9)
    query_weight = scatter_about(seeds[5], (H, DC, QL), QL ** -0.5, 0.15625, ((0, 8), (1, 32)))
    latent_cache = draw_latent_cache(jax.random.fold_in(seeds[15], 71), 0)
    cache_length = with_ends(jax.random.randint(seeds[7], (REQS,), 1, CTX + 1), jax.random.fold_in(seeds[7], 1), 1, CTX).astype(jnp.int32)
    owner_place = jax.random.permutation(seeds[8], REQS).astype(jnp.int32)
    accept_length = with_ends(jax.random.randint(seeds[9], (REQS,), 1, STEPS + 1), jax.random.fold_in(seeds[9], 1), 1, STEPS).astype(jnp.int32)
    value_weight = scatter_about(seeds[10], (H, DL, HV), DL ** -0.5, 0.25, ((0, 8),))
    output_weight = scatter_about(seeds[11], (D, H * HV), (H * HV) ** -0.5, 0.046875, ((0, 32), (1, 8)))
    final_gain = jnp.clip(1.0 + 0.18 * jax.random.normal(seeds[12], (D,), jnp.float32), 0.1, 1.9)
    head_weight = draw_head_weight(jax.random.fold_in(seeds[15], 71), 0)
    draft_tokens = with_ends(ranked_ids(seeds[14], (REQS, STEPS), VOCAB, 2), jax.random.fold_in(seeds[14], 3), 0, VOCAB - 1).astype(jnp.int32)
    return {"hidden_state": hidden_state, "attention_gain": attention_gain, "down_weight": down_weight, "query_gain": query_gain, "latent_gain": latent_gain, "query_weight": query_weight, "latent_cache": latent_cache, "cache_length": cache_length, "owner_place": owner_place, "accept_length": accept_length, "value_weight": value_weight, "output_weight": output_weight, "final_gain": final_gain, "head_weight": head_weight, "draft_tokens": draft_tokens}


epsilon = 1e-06
score_scale = 192.0 ** (-0.5)
masked_score = -1e+30

def row_norm(values, gain_vector):
    inverse_rms = lax.rsqrt(lax.optimization_barrier(jnp.mean(values * values, axis=-1, keepdims=True)) + epsilon)
    return values * inverse_rms * gain_vector

def round_keep(values):
    return lax.optimization_barrier(values.astype(jnp.bfloat16)).astype(jnp.float32)

def attend_request(packed, latent_cache, cache_length):
    query_rows, fresh_block, cache_slot = packed
    cached = latent_cache[cache_slot].astype(jnp.float32)
    length = cache_length[cache_slot]
    query_wide = query_rows.astype(jnp.float32)
    fresh_wide = fresh_block.astype(jnp.float32)
    old_scores = jnp.einsum('shc,pc->shp', query_wide, cached) * score_scale
    live_mask = jnp.arange(cached.shape[0], dtype=jnp.int32) < length
    old_scores = jnp.where(live_mask[None, None, :], old_scores, masked_score)
    new_scores = jnp.einsum('shc,kc->shk', query_wide, fresh_wide) * score_scale
    step_index = jnp.arange(fresh_block.shape[0], dtype=jnp.int32)
    causal = step_index[None, :] <= step_index[:, None]
    new_scores = jnp.where(causal[:, None, :], new_scores, masked_score)
    row_peak = jnp.maximum(lax.optimization_barrier(jnp.max(old_scores, axis=-1)), lax.optimization_barrier(jnp.max(new_scores, axis=-1)))
    old_exp = jnp.exp(old_scores - row_peak[..., None])
    new_exp = jnp.exp(new_scores - row_peak[..., None])
    exp_total = lax.optimization_barrier(jnp.sum(old_exp, axis=-1)) + lax.optimization_barrier(jnp.sum(new_exp, axis=-1))
    old_weight = round_keep(old_exp / exp_total[..., None])
    new_weight = round_keep(new_exp / exp_total[..., None])
    mixed_values = jnp.einsum('shp,pc->shc', old_weight, cached[:, :DL])
    mixed_values = mixed_values + jnp.einsum('shk,kc->shc', new_weight, fresh_wide[:, :DL])
    return mixed_values.astype(jnp.bfloat16)

def reference(hidden_state, attention_gain, down_weight, query_gain, latent_gain, query_weight, latent_cache, cache_length, owner_place, accept_length, value_weight, output_weight, final_gain, head_weight, draft_tokens):
    stream = hidden_state.astype(jnp.float32)
    scaled = (stream * attention_gain[:, None]).astype(jnp.bfloat16)
    projected = lax.dot_general(scaled, down_weight, (((0,), (0,)), ((), ())), preferred_element_type=jnp.float32)
    inverse_norm = lax.rsqrt(lax.optimization_barrier(jnp.sum(stream * stream, axis=0)) / D + epsilon)
    latent = projected * inverse_norm[:, None]
    query_latent = row_norm(latent[:, :QL], query_gain).astype(jnp.bfloat16)
    latent_part = row_norm(latent[:, QL:QL + DL], latent_gain)
    fresh_rows = jnp.concatenate([latent_part, latent[:, QL + DL:]], axis=1).astype(jnp.bfloat16)
    queries = jnp.einsum('rq,hcq->rhc', query_latent.astype(jnp.float32), query_weight.astype(jnp.float32)).astype(jnp.bfloat16)
    queries = queries.reshape(REQS, STEPS, H, DL + DR)
    fresh_blocks = fresh_rows.reshape(REQS, STEPS, DL + DR)
    attended = lax.map(lambda packed: attend_request(packed, latent_cache, cache_length), (queries, fresh_blocks, owner_place))
    head_values = jnp.einsum('ushc,hcv->ushv', attended.astype(jnp.float32), value_weight.astype(jnp.float32)).astype(jnp.bfloat16)
    head_values = head_values.reshape(ROWS, H * HV)
    attn_output = lax.dot_general(output_weight, head_values, (((1,), (1,)), ((), ())), preferred_element_type=jnp.float32)
    residual = round_keep(stream + attn_output)
    normed = residual * lax.rsqrt(lax.optimization_barrier(jnp.sum(residual * residual, axis=0)) / D + epsilon)[None, :] * final_gain[:, None]
    normed = normed.astype(jnp.bfloat16)
    logits = lax.dot_general(normed, head_weight, (((0,), (0,)), ((), ())), preferred_element_type=jnp.float32)
    row_peak = lax.optimization_barrier(jnp.max(logits, axis=1))
    log_total = row_peak + jnp.log(lax.optimization_barrier(jnp.sum(jnp.exp(logits - row_peak[:, None]), axis=1)))
    accepted = (jnp.arange(STEPS, dtype=jnp.int32)[None, :] < accept_length[:, None]).reshape(ROWS)
    log_probs = jnp.where(accepted[:, None], logits - log_total[:, None], jnp.zeros_like(logits))
    target = jnp.take_along_axis(logits, draft_tokens.reshape(ROWS, 1).astype(jnp.int32), axis=1)[:, 0]
    draft_scores = jnp.where(accepted, target - log_total, jnp.zeros_like(target))
    kept_rows = jnp.where(accepted[:, None], fresh_rows, jnp.zeros_like(fresh_rows)).reshape(REQS, STEPS, DL + DR)
    committed = jnp.zeros_like(kept_rows).at[owner_place].set(kept_rows)
    return (log_probs, draft_scores, committed)
```

```python
import jax
import jax.numpy as jnp
from jax import lax
from jax.experimental import pallas as pl
from jax.experimental.pallas import tpu as pltpu
from jax.sharding import Mesh, PartitionSpec as P

D = 7168
QL = 1536
DL = 512
DR = 64
DC = DL + DR
CTX = 4096
NX, NZ, NY, NC = 4, 8, 4, 2
DP = ("x", "z")
TP = ("y", "c")
CHUNK = 1024

epsilon = 1e-06
score_scale = 192.0 ** (-0.5)
masked_score = -1e30


def row_norm(values, gain_vector):
    inverse_rms = lax.rsqrt(jnp.mean(values * values, axis=-1, keepdims=True) + epsilon)
    return values * inverse_rms * gain_vector


def share(block, axes, count):
    copies = jnp.broadcast_to(block[None], (count,) + block.shape)
    return lax.all_to_all(copies, axes, split_axis=0, concat_axis=0, tiled=True)


def swap_cores(block):
    return lax.ppermute(block, "c", [(0, 1), (1, 0)])


def attend_kernel(length_ref, q_ref, fresh_ref, kt_hbm, out_ref, kbuf, sbuf, sems):
    slots, rows, _ = q_ref.shape
    chunks = CTX // CHUNK

    def copy(slot, chunk):
        start = chunk * CHUNK
        if not isinstance(start, int):
            start = pl.multiple_of(start, CHUNK)
        return pltpu.make_async_copy(
            kt_hbm.at[slot, :, pl.ds(start, CHUNK)], kbuf.at[slot, chunk], sems.at[slot, chunk]
        )

    for slot in range(slots):
        for chunk in range(chunks):

            @pl.when(chunk * CHUNK < length_ref[slot])
            def _():
                copy(slot, chunk).start()

    def one_slot(slot, carry):
        length = length_ref[slot]
        live = (length + (CHUNK - 1)) // CHUNK
        q = q_ref[slot]
        fresh = fresh_ref[slot]
        new = lax.dot_general(q, fresh, (((1,), (1,)), ((), ())), preferred_element_type=jnp.float32)
        new = new * score_scale
        key_at = lax.broadcasted_iota(jnp.int32, new.shape, 1)
        step_at = lax.broadcasted_iota(jnp.int32, new.shape, 0) // (rows // 2)
        new = jnp.where(key_at <= step_at, new, masked_score)

        def score(chunk, peak):
            copy(slot, chunk).wait()
            s = jnp.dot(q, kbuf[slot, chunk], preferred_element_type=jnp.float32) * score_scale
            at = chunk * CHUNK + lax.broadcasted_iota(jnp.int32, s.shape, 1)
            s = jnp.where(at < length, s, masked_score)
            sbuf[chunk] = s
            for lane in range(0, CHUNK, 128):
                peak = jnp.maximum(peak, s[:, lane : lane + 128])
            return peak

        peak = lax.fori_loop(0, live, score, jnp.full((rows, 128), masked_score, jnp.float32))
        peak = jnp.maximum(
            jnp.max(peak, axis=-1, keepdims=True), jnp.max(new, axis=-1, keepdims=True)
        )
        new = jnp.exp(new - peak)

        def lift(chunk, total):
            e = jnp.exp(sbuf[chunk] - peak)
            sbuf[chunk] = e
            for lane in range(0, CHUNK, 128):
                total = total + e[:, lane : lane + 128]
            return total

        total = lax.fori_loop(0, live, lift, jnp.zeros((rows, 128), jnp.float32))
        total = jnp.sum(total, axis=-1, keepdims=True) + jnp.sum(new, axis=-1, keepdims=True)
        inverse = 1.0 / total
        mixed = jnp.dot(
            (new * inverse).astype(jnp.bfloat16), fresh[:, :DL], preferred_element_type=jnp.float32
        )

        def mix(chunk, acc):
            weight = (sbuf[chunk] * inverse).astype(jnp.bfloat16)
            return acc + lax.dot_general(
                weight,
                kbuf[slot, chunk, :DL, :],
                (((1,), (1,)), ((), ())),
                preferred_element_type=jnp.float32,
            )

        mixed = lax.fori_loop(0, live, mix, mixed)
        out_ref[slot] = mixed.astype(jnp.bfloat16)
        return carry

    lax.fori_loop(0, slots, one_slot, 0)


def attend(lengths, q, fresh, cache):
    slots, rows, _ = q.shape
    keys = jnp.swapaxes(cache, 1, 2)
    return pl.pallas_call(
        attend_kernel,
        out_shape=jax.ShapeDtypeStruct((slots, rows, DL), jnp.bfloat16),
        grid_spec=pltpu.PrefetchScalarGridSpec(
            num_scalar_prefetch=1,
            grid=(1,),
            in_specs=[
                pl.BlockSpec(q.shape, lambda i, n: (0, 0, 0)),
                pl.BlockSpec(fresh.shape, lambda i, n: (0, 0, 0)),
                pl.BlockSpec(memory_space=pl.ANY),
            ],
            out_specs=pl.BlockSpec((slots, rows, DL), lambda i, n: (0, 0, 0)),
            scratch_shapes=[
                pltpu.VMEM((slots, CTX // CHUNK, DC, CHUNK), jnp.bfloat16),
                pltpu.VMEM((CTX // CHUNK, rows, CHUNK), jnp.float32),
                pltpu.SemaphoreType.DMA((slots, CTX // CHUNK)),
            ],
        ),
        compiler_params=pltpu.CompilerParams(vmem_limit_bytes=44 * 1024 * 1024),
        name="attend",
    )(lengths, q, fresh, keys)


HALF = D // (NX * NZ * NC)


def head_kernel(core_ref, own_ref, other_ref, gain_ref, weight_hbm, out_ref, wbuf, nbuf, sem):
    core = core_ref[0]
    copies = [
        pltpu.make_async_copy(weight_hbm.at[x], wbuf.at[x], sem.at[x]) for x in range(NX)
    ]
    for copy in copies:
        copy.start()
    gain = jnp.transpose(gain_ref[...])
    inverse = []
    for y in range(NY):

        def squares(x, acc):
            for ref in (own_ref, other_ref):
                for z in range(NZ):
                    v = ref[x, y, z].astype(jnp.float32)
                    acc = acc + jnp.sum((v * v).reshape(HALF // 8, 8, 128), axis=0)
            return acc

        acc = lax.fori_loop(0, NX, squares, jnp.zeros((8, 128), jnp.float32))
        inverse.append(lax.rsqrt(jnp.sum(acc, axis=0, keepdims=True) / D + epsilon))
    for x in range(NX):
        copies[x].wait()
        for half, ref in ((core, own_ref), (1 - core, other_ref)):
            for z in range(NZ):
                at = (x * NZ + z) * NC
                column = jnp.where(half == 0, gain[:, at : at + 1], gain[:, at + 1 : at + 2])
                for y in range(NY):
                    v = ref[x, y, z].astype(jnp.float32)
                    nbuf[y, z] = (v * inverse[y] * column).astype(jnp.bfloat16)
            weight = wbuf[x, :, half].reshape(NZ * HALF, wbuf.shape[-1])
            for y in range(NY):
                part = lax.dot_general(
                    nbuf[y].reshape(NZ * HALF, 128),
                    weight,
                    (((0,), (0,)), ((), ())),
                    preferred_element_type=jnp.float32,
                )
                if x == 0 and ref is own_ref:
                    out_ref[y] = part
                else:
                    out_ref[y] += part


def head(core, own, other, gain, weight):
    width = weight.shape[1]
    weight = weight.reshape(NX, NZ, NC, HALF, width)
    vmem = pl.BlockSpec(memory_space=pltpu.VMEM)
    return pl.pallas_call(
        head_kernel,
        out_shape=jax.ShapeDtypeStruct((NY, 128, width), jnp.float32),
        in_specs=[
            pl.BlockSpec(memory_space=pltpu.SMEM),
            vmem,
            vmem,
            vmem,
            pl.BlockSpec(memory_space=pl.ANY),
        ],
        out_specs=vmem,
        scratch_shapes=[
            pltpu.VMEM(weight.shape, jnp.bfloat16),
            pltpu.VMEM((NY, NZ, HALF, 128), jnp.bfloat16),
            pltpu.SemaphoreType.DMA((NX,)),
        ],
        compiler_params=pltpu.CompilerParams(vmem_limit_bytes=32 * 1024 * 1024),
        name="head",
    )(core, own, other, gain.reshape(NX * NZ * NC, HALF), weight)


def merge(peak, total, hit):
    top = jnp.max(peak, axis=0)
    return top, jnp.sum(total * jnp.exp(peak - top[None]), axis=0), jnp.sum(hit, axis=0)


def on_device(
    hidden_state,
    attention_gain,
    down_weight,
    query_gain,
    latent_gain,
    query_weight,
    latent_cache,
    cache_length,
    owner_place,
    accept_length,
    value_weight,
    output_weight,
    final_gain,
    head_weight,
    draft_tokens,
):
    x, z, y, c = (lax.axis_index(a) for a in ("x", "z", "y", "c"))
    d = x * NZ + z
    t = y * NC + c
    dp_count, tp_count = NX * NZ, NY * NC
    request_count, step_count = draft_tokens.shape
    row_count = request_count * step_count
    local_requests = latent_cache.shape[0]
    local_rows = local_requests * step_count
    slice_width = query_weight.shape[1]
    local_heads, _, value_width = value_weight.shape
    own_rows = local_rows // tp_count
    step_index = jnp.arange(step_count, dtype=jnp.int32)

    stream = hidden_state.astype(jnp.float32)
    scaled = (stream * attention_gain[:, None]).astype(jnp.bfloat16)
    column_part = lax.dot_general(
        scaled, down_weight, (((0,), (0,)), ((), ())), preferred_element_type=jnp.float32
    )
    inverse_norm = lax.rsqrt(jnp.sum(stream * stream, axis=0) / D + epsilon)
    column_part = column_part * inverse_norm[:, None]
    latent = lax.all_to_all(
        column_part.reshape(tp_count, own_rows, -1), TP, split_axis=0, concat_axis=0, tiled=True
    )
    latent = jnp.swapaxes(latent, 0, 1).reshape(own_rows, QL + DC)
    query_latent = row_norm(latent[:, :QL], query_gain)
    latent_part = row_norm(latent[:, QL : QL + DL], latent_gain)
    rows = jnp.concatenate([query_latent, latent_part, latent[:, QL + DL :]], axis=1)
    rows = rows.astype(jnp.bfloat16)

    rows = share(rows, "z", NZ).reshape(NZ * own_rows, QL + DC)
    rows = share(rows, ("x", "y"), NX * NY).reshape(row_count // NC, QL + DC)
    other_rows = swap_cores(rows)
    place = jnp.arange(row_count // NC, dtype=jnp.int32)
    at_i = place % own_rows
    at_z = place // own_rows % NZ
    at_y = place // (own_rows * NZ) % NY
    at_x = place // (own_rows * NZ * NY)

    def row_ids(core):
        return ((at_x * NZ + at_z) * tp_count + at_y * NC + core) * own_rows + at_i

    request_row = jnp.concatenate([row_ids(c), row_ids(1 - c)])

    weight = jnp.swapaxes(query_weight, 0, 1).reshape(slice_width * local_heads, QL)

    def project(block):
        part = lax.dot_general(
            block[:, :QL], weight, (((1,), (1,)), ((), ())), preferred_element_type=jnp.float32
        )
        return part.astype(jnp.bfloat16)

    query_part = jnp.concatenate([project(rows), project(other_rows)])
    every_fresh = jnp.concatenate([rows[:, QL:], other_rows[:, QL:]])
    owner_row = (owner_place[:, None] * step_count + step_index[None, :]).reshape(row_count)
    slot_of_place = jnp.zeros((row_count,), jnp.int32)
    row_index = jnp.arange(row_count, dtype=jnp.int32)
    same = request_row[None, :] == row_index[:, None]
    slot_of_place = jnp.sum(jnp.where(same, owner_row[:, None], 0), axis=0)
    reorder = (slot_of_place[None, :] == row_index[:, None]).astype(jnp.bfloat16)
    query_owned = jnp.dot(reorder, query_part, preferred_element_type=jnp.float32)
    query_owned = query_owned.astype(jnp.bfloat16).reshape(dp_count, local_rows, -1)
    own_reorder = (
        slot_of_place[None, :] == (d * local_rows + jnp.arange(local_rows, dtype=jnp.int32))[:, None]
    ).astype(jnp.bfloat16)
    own_fresh = jnp.dot(own_reorder, every_fresh, preferred_element_type=jnp.float32)
    own_fresh = own_fresh.astype(jnp.bfloat16).reshape(local_requests, step_count, DC)

    lane_rows = local_rows // NY
    mine = hidden_state.reshape(dp_count, NC, HALF, NY, lane_rows)
    mine = lax.dynamic_index_in_dim(mine, c, 1, keepdims=False)
    mine = lax.dynamic_index_in_dim(mine, y, 2, keepdims=False)
    mine = mine.reshape(dp_count, local_rows, HALF * lane_rows // local_rows)
    width = slice_width * local_heads
    arrived = lax.all_to_all(
        jnp.concatenate([query_owned, mine], axis=2), DP, split_axis=0, concat_axis=0, tiled=True
    )
    stream_block = arrived[:, :, width:].reshape(dp_count, HALF, lane_rows)
    stream_block = jnp.transpose(stream_block, (1, 0, 2)).reshape(HALF, dp_count * lane_rows)
    arrived = arrived[:, :, :width].reshape(
        dp_count, local_requests, step_count, slice_width, local_heads
    )
    queries = jnp.transpose(arrived, (1, 2, 4, 0, 3)).reshape(
        local_requests, step_count * local_heads, DC
    )

    fresh_padded = jnp.pad(own_fresh, ((0, 0), (0, 16 - step_count), (0, 0)))
    attended = attend(cache_length, queries, fresh_padded, latent_cache)
    attended = attended.reshape(local_requests, step_count, local_heads, DL)
    head_values = jnp.einsum(
        "ushc,hcv->ushv", attended, value_weight, preferred_element_type=jnp.float32
    )
    head_values = head_values.astype(jnp.bfloat16).reshape(local_rows, local_heads * value_width)
    head_values = share(head_values, "z", NZ).reshape(NZ * local_rows, -1)
    head_values = share(head_values, "x", NX).reshape(row_count, -1)

    turned = row_index.reshape(dp_count, NY, lane_rows).swapaxes(0, 1).reshape(row_count)
    turned_owner = owner_row.reshape(dp_count, NY, lane_rows).swapaxes(0, 1).reshape(row_count)
    turn = (turned_owner[:, None] == row_index[None, :]).astype(jnp.bfloat16)
    head_values = jnp.dot(turn, head_values, preferred_element_type=jnp.float32)
    head_values = head_values.astype(jnp.bfloat16)
    terms = lax.dot_general(
        output_weight, head_values, (((1,), (1,)), ((), ())), preferred_element_type=jnp.float32
    )
    terms = terms.reshape(NC, HALF, row_count)
    kept = lax.dynamic_index_in_dim(terms, c, 0, keepdims=False)
    sent = lax.dynamic_index_in_dim(terms, 1 - c, 0, keepdims=False)
    kept = kept + swap_cores(sent)
    kept = jnp.swapaxes(kept.reshape(HALF, NY, row_count // NY), 0, 1)
    kept = lax.all_to_all(kept, "y", split_axis=0, concat_axis=0, tiled=True)
    residual = (jnp.sum(kept, axis=0) + stream_block.astype(jnp.float32)).astype(jnp.bfloat16)

    residual = share(residual, "z", NZ)
    residual = share(residual, ("x", "y"), NX * NY)
    residual = residual.reshape(NX, NY, NZ, HALF, row_count // NY)
    other = swap_cores(residual)
    logits = head(c.reshape(1), residual, other, final_gain, head_weight)

    vocab_width = head_weight.shape[1]
    logits = logits.reshape(row_count, vocab_width)
    vocab_start = (d * tp_count + t) * vocab_width

    def turn_rows(flat):
        return flat.reshape(dp_count, NY, lane_rows).swapaxes(0, 1).reshape(row_count)

    target_hit = (turn_rows(draft_tokens) - vocab_start)[:, None] == jnp.arange(
        vocab_width, dtype=jnp.int32
    )[None, :]
    hit = jnp.sum(jnp.where(target_hit, logits, jnp.zeros_like(logits)), axis=1)
    peak = jnp.max(logits, axis=1)
    total = jnp.sum(jnp.exp(logits - peak[:, None]), axis=1)
    stats = jnp.stack([peak, total, hit]).reshape(3, NY, 128)
    stats = jnp.stack([stats, swap_cores(stats)])
    stats = jnp.stack(merge(stats[:, 0], stats[:, 1], stats[:, 2]))
    stats = share(stats, "y", NY)
    stats = jnp.stack(merge(stats[:, 0], stats[:, 1], stats[:, 2]))
    stats = share(stats, DP, dp_count)
    peak, total, target = merge(stats[:, 0], stats[:, 1], stats[:, 2])
    log_total = (peak + jnp.log(total)).reshape(row_count)
    target = target.reshape(row_count)
    accepted = turn_rows((step_index[None, :] < accept_length[:, None]).reshape(row_count))
    log_probs = jnp.where(accepted[:, None], logits - log_total[:, None], jnp.zeros_like(logits))
    draft_scores = jnp.where(accepted, target - log_total, jnp.zeros_like(target))

    def back(turned_rows):
        shape = turned_rows.shape[1:]
        turned_rows = turned_rows.reshape((NY, dp_count, lane_rows) + shape)
        return jnp.swapaxes(turned_rows, 0, 1).reshape((row_count,) + shape)

    slot_global = d * local_requests + jnp.arange(local_requests, dtype=jnp.int32)
    slot_match = owner_place[None, :] == slot_global[:, None]
    slot_accept = jnp.sum(
        jnp.where(slot_match, accept_length[None, :], jnp.zeros_like(slot_match, dtype=jnp.int32)),
        axis=1,
    )
    keep_mask = step_index[None, :, None] < slot_accept[:, None, None]
    committed = jnp.where(keep_mask, own_fresh, jnp.zeros_like(own_fresh))
    return (back(log_probs), back(draft_scores), committed)


def solution(mesh):
    split = Mesh(mesh.devices.reshape(NX, NZ, NY, NC), ("x", "z", "y", "c"))
    return jax.shard_map(
        on_device,
        mesh=split,
        in_specs=(
            P(None, DP),
            P(),
            P(None, TP),
            P(),
            P(),
            P(TP, DP, None),
            P(DP, None, None),
            P(DP),
            P(),
            P(),
            P(TP, None, None),
            P(DP, TP),
            P(),
            P(None, DP + TP),
            P(),
        ),
        out_specs=(P(None, DP + TP), P(), P(DP, None, None)),
        check_vma=False,
    )
```

```python
import jax
import jax.numpy as jnp
from jax import lax
from jax.experimental import pallas as pl
from jax.experimental.pallas import tpu as pltpu
from jax.sharding import Mesh, PartitionSpec as P

D = 7168
QL = 1536
DL = 512
DR = 64
DC = DL + DR
CTX = 4096
NX, NZ, NY, NC = 4, 8, 4, 2
DP = ("x", "z")
TP = ("y", "c")
CHUNK = 1024
PAD = 64
REL = (0, 3, 1, 2)

epsilon = 1e-06
score_scale = 192.0 ** (-0.5)
masked_score = -1e30


def row_norm(values, gain_vector):
    inverse_rms = lax.rsqrt(jnp.mean(values * values, axis=-1, keepdims=True) + epsilon)
    return values * inverse_rms * gain_vector


def share(block, axes, count):
    copies = jnp.broadcast_to(block[None], (count,) + block.shape)
    return lax.all_to_all(copies, axes, split_axis=0, concat_axis=0, tiled=True)


def swap_cores(block):
    return lax.ppermute(block, "c", [(0, 1), (1, 0)])


def shift(block, axis, step):
    return lax.ppermute(block, axis, [(i, (i + step) % 4) for i in range(4)])


def ring(block, axis):
    half = block.shape[0] // 2
    before = shift(block, axis, 1)
    after = shift(block, axis, -1)
    return block, before, after, shift(before[:half], axis, 1), shift(after[half:], axis, -1)


def attend_kernel(length_ref, xt_ref, fresh_ref, kt_hbm, out_ref, kbuf, sbuf, qbuf, sems):
    slots, rows, _ = out_ref.shape
    chunks = CTX // CHUNK
    row_count, packed, sources = xt_ref.shape
    heads = slots * rows // row_count
    width = packed // heads

    def copy(slot, chunk):
        start = chunk * CHUNK
        if not isinstance(start, int):
            start = pl.multiple_of(start, CHUNK)
        return pltpu.make_async_copy(
            kt_hbm.at[slot, :, pl.ds(start, CHUNK)], kbuf.at[slot, chunk], sems.at[slot, chunk]
        )

    for slot in range(slots):
        for chunk in range(chunks):

            @pl.when(chunk * CHUNK < length_ref[slot])
            def _():
                copy(slot, chunk).start()

    pieces = [
        xt_ref[:, w * heads : (w + 1) * heads, :].reshape(slots * rows, sources)
        for w in range(width)
    ]
    source = lax.broadcasted_iota(jnp.int32, (DC, DC), 0)
    target = lax.broadcasted_iota(jnp.int32, (DC, DC), 1)
    order = target == (source % sources) * width + source // sources
    order = jnp.where(order, 1.0, 0.0).astype(jnp.bfloat16)
    q_all = jnp.dot(
        jnp.concatenate(pieces, axis=1), order, preferred_element_type=jnp.float32
    ).astype(jnp.bfloat16)
    qbuf[...] = q_all.reshape(slots, rows, DC)

    def one_slot(slot, carry):
        length = length_ref[slot]
        live = (length + (CHUNK - 1)) // CHUNK
        q = qbuf[slot]
        fresh = fresh_ref[slot]
        new = lax.dot_general(q, fresh, (((1,), (1,)), ((), ())), preferred_element_type=jnp.float32)
        new = new * score_scale
        key_at = lax.broadcasted_iota(jnp.int32, new.shape, 1)
        step_at = lax.broadcasted_iota(jnp.int32, new.shape, 0) // (rows // 2)
        new = jnp.where(key_at <= step_at, new, masked_score)

        def score(chunk, peak):
            copy(slot, chunk).wait()
            s = jnp.dot(q, kbuf[slot, chunk], preferred_element_type=jnp.float32) * score_scale
            at = chunk * CHUNK + lax.broadcasted_iota(jnp.int32, s.shape, 1)
            s = jnp.where(at < length, s, masked_score)
            sbuf[chunk] = s
            for lane in range(0, CHUNK, 128):
                peak = jnp.maximum(peak, s[:, lane : lane + 128])
            return peak

        peak = lax.fori_loop(0, live, score, jnp.full((rows, 128), masked_score, jnp.float32))
        peak = jnp.maximum(
            jnp.max(peak, axis=-1, keepdims=True), jnp.max(new, axis=-1, keepdims=True)
        )
        new = jnp.exp(new - peak)

        def lift(chunk, total):
            e = jnp.exp(sbuf[chunk] - peak)
            sbuf[chunk] = e
            for lane in range(0, CHUNK, 128):
                total = total + e[:, lane : lane + 128]
            return total

        total = lax.fori_loop(0, live, lift, jnp.zeros((rows, 128), jnp.float32))
        total = jnp.sum(total, axis=-1, keepdims=True) + jnp.sum(new, axis=-1, keepdims=True)
        inverse = 1.0 / total
        mixed = jnp.dot(
            (new * inverse).astype(jnp.bfloat16), fresh[:, :DL], preferred_element_type=jnp.float32
        )

        def mix(chunk, acc):
            weight = (sbuf[chunk] * inverse).astype(jnp.bfloat16)
            return acc + lax.dot_general(
                weight,
                kbuf[slot, chunk, :DL, :],
                (((1,), (1,)), ((), ())),
                preferred_element_type=jnp.float32,
            )

        mixed = lax.fori_loop(0, live, mix, mixed)
        out_ref[slot] = mixed.astype(jnp.bfloat16)
        return carry

    lax.fori_loop(0, slots, one_slot, 0)


def attend(lengths, packed, fresh, cache):
    slots = cache.shape[0]
    rows = packed.shape[0] * (packed.shape[1] * packed.shape[2] // DC) // slots
    keys = jnp.swapaxes(cache, 1, 2)
    return pl.pallas_call(
        attend_kernel,
        out_shape=jax.ShapeDtypeStruct((slots, rows, DL), jnp.bfloat16),
        grid_spec=pltpu.PrefetchScalarGridSpec(
            num_scalar_prefetch=1,
            grid=(1,),
            in_specs=[
                pl.BlockSpec(packed.shape, lambda i, n: (0, 0, 0)),
                pl.BlockSpec(fresh.shape, lambda i, n: (0, 0, 0)),
                pl.BlockSpec(memory_space=pl.ANY),
            ],
            out_specs=pl.BlockSpec((slots, rows, DL), lambda i, n: (0, 0, 0)),
            scratch_shapes=[
                pltpu.VMEM((slots, CTX // CHUNK, DC, CHUNK), jnp.bfloat16),
                pltpu.VMEM((CTX // CHUNK, rows, CHUNK), jnp.float32),
                pltpu.VMEM((slots, rows, DC), jnp.bfloat16),
                pltpu.SemaphoreType.DMA((slots, CTX // CHUNK)),
            ],
        ),
        compiler_params=pltpu.CompilerParams(vmem_limit_bytes=46 * 1024 * 1024),
        name="attend",
    )(lengths, packed, fresh, keys)


HALF = D // (NX * NZ * NC)


PIECES = 5


def piece_of(refs, k, m, group):
    outer, inner = (m, k) if group == 0 else (k, m)
    refs = refs[group * PIECES : (group + 1) * PIECES]
    if outer < 3:
        return refs[outer], inner
    if inner < 2:
        return refs[3], inner
    return refs[4], inner - 2


def head_kernel(place_ref, gain_ref, weight_hbm, other_hbm, *rest):
    refs, rest = rest[: 2 * PIECES], rest[2 * PIECES :]
    out_ref, wbuf, abuf, bbuf, nbuf, wsem, sem = rest
    x0, y0, core = place_ref[0], place_ref[1], place_ref[2]
    bufs = abuf, bbuf

    def block_copy(group, k, m):
        ref, at = piece_of(refs, k, m, group)
        return pltpu.make_async_copy(ref.at[at], bufs[group].at[k, m], sem.at[group, k, m])

    def weight_copies(k):
        at = (x0 + REL[k]) % NX
        return (
            pltpu.make_async_copy(weight_hbm.at[at, :, core], wbuf.at[k, 0], wsem.at[k, 0]),
            pltpu.make_async_copy(other_hbm.at[at], wbuf.at[k, 1], wsem.at[k, 1]),
        )

    for k in range(NX):
        for m in range(NY):
            block_copy(0, k, m).start()
    for k in range(NX):
        for m in range(NY):
            block_copy(1, k, m).start()
        for copy in weight_copies(k):
            copy.start()
    for k in range(NX):
        for m in range(NY):
            block_copy(0, k, m).wait()
    inverse = []
    for m in range(NY):
        total = jnp.zeros((16, 128), jnp.float32)
        for k in range(NX):
            total = total + abuf[k, m, NZ // 2 * HALF :, :].astype(jnp.float32)
        inverse.append(lax.rsqrt(jnp.sum(total, axis=0, keepdims=True) / D + epsilon))
    for k in range(NX):
        gain = jnp.transpose(gain_ref[(x0 + REL[k]) % NX, core])
        for m in range(NY):
            block_copy(1, k, m).wait()
        for z in range(NZ):
            column = gain[:, z : z + 1]
            at = z % (NZ // 2) * HALF
            for m in range(NY):
                v = bufs[z // (NZ // 2)][k, m, at : at + HALF, :].astype(jnp.float32)
                nbuf[k % 2, m, z] = (v * inverse[m] * column).astype(jnp.bfloat16)
        for copy in weight_copies(k):
            copy.wait()
        for part in range(NC):
            weight = wbuf[k, part].reshape(NZ * HALF, wbuf.shape[-1])
            for m in range(NY):
                term = lax.dot_general(
                    nbuf[k % 2, m].reshape(NZ * HALF, 128),
                    weight,
                    (((0,), (0,)), ((), ())),
                    preferred_element_type=jnp.float32,
                )
                at = (y0 + REL[m]) % NY
                if k == 0:
                    out_ref[part, at] = term
                else:
                    out_ref[part, at] += term


def head(place, gain, weight, other, pieces):
    width = weight.shape[-1]
    vmem = pl.BlockSpec(memory_space=pltpu.VMEM)
    far = pl.BlockSpec(memory_space=pltpu.HBM)
    gain = jnp.transpose(gain.reshape(NX, NZ, NC, HALF), (0, 2, 1, 3))
    return pl.pallas_call(
        head_kernel,
        out_shape=jax.ShapeDtypeStruct((NC, NY, 128, width), jnp.float32),
        in_specs=[pl.BlockSpec(memory_space=pltpu.SMEM), vmem, far, far] + [far] * len(pieces),
        out_specs=vmem,
        scratch_shapes=[
            pltpu.VMEM((NX, NC, NZ, HALF, width), jnp.bfloat16),
            pltpu.VMEM((NX, NY) + pieces[0].shape[1:], jnp.bfloat16),
            pltpu.VMEM((NX, NY) + pieces[PIECES].shape[1:], jnp.bfloat16),
            pltpu.VMEM((2, NY, NZ, HALF, 128), jnp.bfloat16),
            pltpu.SemaphoreType.DMA((NX, NC)),
            pltpu.SemaphoreType.DMA((2, NX, NY)),
        ],
        compiler_params=pltpu.CompilerParams(vmem_limit_bytes=60 * 1024 * 1024),
        name="head",
    )(place, gain, weight, other, *pieces)


def project_kernel(
    slot_ref, mine_ref, rows_ref, other_ref, weight_ref, stream_ref, out_ref, fresh_ref
):
    count = slot_ref.shape[1]
    half = count // NC
    width = weight_ref.shape[0]
    total = None
    fresh = None
    for part, ref in enumerate((rows_ref, other_ref)):
        term = lax.dot_general(
            ref[:, :QL], weight_ref[...], (((1,), (1,)), ((), ())),
            preferred_element_type=jnp.float32,
        ).astype(jnp.bfloat16)
        slot = slot_ref[:, part * half : (part + 1) * half]
        wanted = lax.broadcasted_iota(jnp.int32, (count, half), 0)
        pick = jnp.where(slot == wanted, 1.0, 0.0).astype(jnp.bfloat16)
        term = jnp.dot(pick, term, preferred_element_type=jnp.float32)
        total = term if total is None else total + term
        local = fresh_ref.shape[0]
        wanted = lax.broadcasted_iota(jnp.int32, (local, half), 0) + mine_ref[0]
        pick = jnp.where(slot == wanted, 1.0, 0.0).astype(jnp.bfloat16)
        term = jnp.dot(pick, ref[:, QL : QL + DC], preferred_element_type=jnp.float32)
        fresh = term if fresh is None else fresh + term
    fresh_ref[...] = fresh.astype(jnp.bfloat16)
    out_ref[:, :width] = total.astype(jnp.bfloat16)
    local = fresh_ref.shape[0]
    lane_rows = local // NY
    piece = HALF // NY
    hidden = stream_ref[...].astype(jnp.float32)
    chosen = hidden[:lane_rows]
    for y in range(1, NY):
        chosen = jnp.where(mine_ref[1] == y, hidden[y * lane_rows : (y + 1) * lane_rows], chosen)
    for dest in range(NX * NZ):
        at = dest * NC * HALF
        wide = jnp.where(
            mine_ref[2] == 0, chosen[:, at : at + HALF], chosen[:, at + HALF : at + NC * HALF]
        )
        block = jnp.concatenate([wide[:, q * piece : (q + 1) * piece] for q in range(NY)], axis=0)
        out_ref[dest * local : (dest + 1) * local, width:] = block.astype(jnp.bfloat16)


def project(slot, mine, rows, other, weight, stream):
    count = slot.shape[0]
    local = count // (NX * NZ)
    vmem = pl.BlockSpec(memory_space=pltpu.VMEM)
    return pl.pallas_call(
        project_kernel,
        out_shape=(
            jax.ShapeDtypeStruct((count, weight.shape[0] + HALF // NY), jnp.bfloat16),
            jax.ShapeDtypeStruct((local, DC), jnp.bfloat16),
        ),
        in_specs=[vmem, pl.BlockSpec(memory_space=pltpu.SMEM), vmem, vmem, vmem, vmem],
        out_specs=(vmem, vmem),
        compiler_params=pltpu.CompilerParams(vmem_limit_bytes=32 * 1024 * 1024),
        name="project",
    )(slot.reshape(1, count), mine, rows, other, weight, stream)


def merge(peak, total, hit):
    top = jnp.max(peak, axis=0)
    return top, jnp.sum(total * jnp.exp(peak - top[None]), axis=0), jnp.sum(hit, axis=0)


def on_device(
    hidden_state,
    attention_gain,
    down_weight,
    query_gain,
    latent_gain,
    query_weight,
    latent_cache,
    cache_length,
    owner_place,
    accept_length,
    value_weight,
    output_weight,
    final_gain,
    head_weight,
    draft_tokens,
):
    x, z, y, c = (lax.axis_index(a) for a in ("x", "z", "y", "c"))
    d = x * NZ + z
    t = y * NC + c
    dp_count, tp_count = NX * NZ, NY * NC
    request_count, step_count = draft_tokens.shape
    row_count = request_count * step_count
    local_requests = latent_cache.shape[0]
    local_rows = local_requests * step_count
    slice_width = query_weight.shape[1]
    local_heads, _, value_width = value_weight.shape
    own_rows = local_rows // tp_count
    step_index = jnp.arange(step_count, dtype=jnp.int32)

    stream = hidden_state.astype(jnp.float32)
    scaled = (stream * attention_gain[:, None]).astype(jnp.bfloat16)
    column_part = lax.dot_general(
        scaled, down_weight, (((0,), (0,)), ((), ())), preferred_element_type=jnp.float32
    )
    inverse_norm = lax.rsqrt(jnp.sum(stream * stream, axis=0) / D + epsilon)
    column_part = column_part * inverse_norm[:, None]
    latent = lax.all_to_all(
        column_part.reshape(tp_count, own_rows, -1), TP, split_axis=0, concat_axis=0, tiled=True
    )
    latent = jnp.swapaxes(latent, 0, 1).reshape(own_rows, QL + DC)
    query_latent = row_norm(latent[:, :QL], query_gain)
    latent_part = row_norm(latent[:, QL : QL + DL], latent_gain)
    blank = jnp.zeros((own_rows, PAD), jnp.float32)
    rows = jnp.concatenate([query_latent, latent_part, latent[:, QL + DL :], blank], axis=1)
    rows = rows.astype(jnp.bfloat16)

    rows = share(rows, "z", NZ).reshape(NZ * own_rows, -1)
    rows = share(rows, ("x", "y"), NX * NY).reshape(row_count // NC, -1)
    other_rows = swap_cores(rows)
    place = jnp.arange(row_count // NC, dtype=jnp.int32)
    at_i = place % own_rows
    at_z = place // own_rows % NZ
    at_y = place // (own_rows * NZ) % NY
    at_x = place // (own_rows * NZ * NY)

    def row_ids(core):
        return ((at_x * NZ + at_z) * tp_count + at_y * NC + core) * own_rows + at_i

    request_row = jnp.concatenate([row_ids(c), row_ids(1 - c)])

    weight = jnp.swapaxes(query_weight, 0, 1).reshape(slice_width * local_heads, QL)
    owner_row = (owner_place[:, None] * step_count + step_index[None, :]).reshape(row_count)
    row_index = jnp.arange(row_count, dtype=jnp.int32)
    same = request_row[None, :] == row_index[:, None]
    slot_of_place = jnp.sum(jnp.where(same, owner_row[:, None], 0), axis=0)

    lane_rows = local_rows // NY
    width = slice_width * local_heads
    payload, own_fresh = project(
        slot_of_place,
        jnp.stack([d * local_rows, y, c]),
        rows,
        other_rows,
        weight,
        jnp.swapaxes(hidden_state, 0, 1),
    )
    own_fresh = own_fresh.reshape(local_requests, step_count, DC)
    arrived = lax.all_to_all(
        payload.reshape(dp_count, local_rows, -1), DP, split_axis=0, concat_axis=0, tiled=True
    )
    stream_block = arrived[:, :, width:].reshape(dp_count, NY, lane_rows, HALF // NY)
    stream_block = jnp.transpose(stream_block, (1, 3, 0, 2)).reshape(HALF, dp_count * lane_rows)
    packed = jnp.transpose(arrived[:, :, :width], (1, 2, 0))

    fresh_padded = jnp.pad(own_fresh, ((0, 0), (0, 16 - step_count), (0, 0)))
    attended = attend(cache_length, packed, fresh_padded, latent_cache)
    attended = attended.reshape(local_requests, step_count, local_heads, DL)
    head_values = jnp.einsum(
        "ushc,hcv->ushv", attended, value_weight, preferred_element_type=jnp.float32
    )
    head_values = head_values.astype(jnp.bfloat16).reshape(local_rows, local_heads * value_width)
    head_values = share(head_values, "z", NZ).reshape(NZ * local_rows, -1)
    head_values = jnp.concatenate(
        [head_values]
        + [
            lax.ppermute(head_values, "x", [(i, (i + k) % NX) for i in range(NX)])
            for k in range(1, NX)
        ]
    )

    turned = row_index.reshape(dp_count, NY, lane_rows).swapaxes(0, 1).reshape(row_count)
    turned_owner = owner_row.reshape(dp_count, NY, lane_rows).swapaxes(0, 1).reshape(row_count)
    held = (x - row_index // (NZ * local_rows)) % NX * (NZ * local_rows)
    held = held + row_index % (NZ * local_rows)
    turn = (turned_owner[:, None] == held[None, :]).astype(jnp.bfloat16)
    head_values = jnp.dot(turn, head_values, preferred_element_type=jnp.float32)
    head_values = head_values.astype(jnp.bfloat16)
    terms = lax.dot_general(
        output_weight, head_values, (((1,), (1,)), ((), ())), preferred_element_type=jnp.float32
    )
    terms = terms.reshape(NC, HALF, row_count)
    kept = lax.dynamic_index_in_dim(terms, c, 0, keepdims=False)
    sent = lax.dynamic_index_in_dim(terms, 1 - c, 0, keepdims=False)
    kept = kept + swap_cores(sent)
    kept = jnp.swapaxes(kept.reshape(HALF, NY, row_count // NY), 0, 1)
    kept = lax.all_to_all(kept, "y", split_axis=0, concat_axis=0, tiled=True)
    residual = (jnp.sum(kept, axis=0) + stream_block.astype(jnp.float32)).astype(jnp.bfloat16)

    residual = share(residual, "z", NZ)
    squares = residual.astype(jnp.float32)
    squares = jnp.sum(squares * squares, axis=(0, 1))
    squares = squares + swap_cores(squares)
    high = lax.reduce_precision(squares, 8, 7)
    middle = lax.reduce_precision(squares - high, 8, 7)
    parts = jnp.stack([high, middle, squares - high - middle])
    parts = jnp.pad(parts, ((0, 16 - 3), (0, 0))).astype(jnp.bfloat16)
    residual = residual.reshape(NZ * HALF, -1)
    halves = jnp.concatenate([residual[: NZ // 2 * HALF], parts]), residual[NZ // 2 * HALF :]

    def whole(parts):
        return jnp.stack(parts[:3] + (jnp.concatenate(parts[3:]),))

    pieces = ring(whole(ring(halves[0], "x")), "y") + ring(whole(ring(halves[1], "y")), "x")
    place_of = jnp.stack([x, y, c])
    vocab_width = head_weight.shape[1]
    head_weight = head_weight.reshape(NX, NZ, NC, HALF, vocab_width)
    other = swap_cores(lax.dynamic_index_in_dim(head_weight, 1 - c, 2, keepdims=False))
    logits = head(place_of, final_gain, head_weight, other, pieces)
    logits = logits[0] + swap_cores(logits[1])
    logits = logits.reshape(row_count, vocab_width)
    vocab_start = (d * tp_count + t) * vocab_width

    def turn_rows(flat):
        return flat.reshape(dp_count, NY, lane_rows).swapaxes(0, 1).reshape(row_count)

    target_hit = (turn_rows(draft_tokens) - vocab_start)[:, None] == jnp.arange(
        vocab_width, dtype=jnp.int32
    )[None, :]
    hit = jnp.sum(jnp.where(target_hit, logits, jnp.zeros_like(logits)), axis=1)
    peak = jnp.max(logits, axis=1)
    total = jnp.sum(jnp.exp(logits - peak[:, None]), axis=1)
    stats = jnp.stack([peak, total, hit]).reshape(3, NY, 128)
    stats = jnp.stack([stats, swap_cores(stats)])
    stats = jnp.stack(merge(stats[:, 0], stats[:, 1], stats[:, 2]))
    stats = share(stats, "y", NY)
    stats = jnp.stack(merge(stats[:, 0], stats[:, 1], stats[:, 2]))
    stats = share(stats, DP, dp_count)
    peak, total, target = merge(stats[:, 0], stats[:, 1], stats[:, 2])
    log_total = (peak + jnp.log(total)).reshape(row_count)
    target = target.reshape(row_count)
    accepted = turn_rows((step_index[None, :] < accept_length[:, None]).reshape(row_count))
    log_probs = jnp.where(accepted[:, None], logits - log_total[:, None], jnp.zeros_like(logits))
    draft_scores = jnp.where(accepted, target - log_total, jnp.zeros_like(target))

    def back(turned_rows):
        shape = turned_rows.shape[1:]
        turned_rows = turned_rows.reshape((NY, dp_count, lane_rows) + shape)
        return jnp.swapaxes(turned_rows, 0, 1).reshape((row_count,) + shape)

    slot_global = d * local_requests + jnp.arange(local_requests, dtype=jnp.int32)
    slot_match = owner_place[None, :] == slot_global[:, None]
    slot_accept = jnp.sum(
        jnp.where(slot_match, accept_length[None, :], jnp.zeros_like(slot_match, dtype=jnp.int32)),
        axis=1,
    )
    keep_mask = step_index[None, :, None] < slot_accept[:, None, None]
    committed = jnp.where(keep_mask, own_fresh, jnp.zeros_like(own_fresh))
    return (back(log_probs), back(draft_scores), committed)


def solution(mesh):
    split = Mesh(mesh.devices.reshape(NX, NZ, NY, NC), ("x", "z", "y", "c"))
    return jax.shard_map(
        on_device,
        mesh=split,
        in_specs=(
            P(None, DP),
            P(),
            P(None, TP),
            P(),
            P(),
            P(TP, DP, None),
            P(DP, None, None),
            P(DP),
            P(),
            P(),
            P(TP, None, None),
            P(DP, TP),
            P(),
            P(None, DP + TP),
            P(),
        ),
        out_specs=(P(None, DP + TP), P(), P(DP, None, None)),
        check_vma=False,
    )
```

```python
import jax
import jax.numpy as jnp
from jax import lax
from jax.experimental import pallas as pl
from jax.experimental.pallas import tpu as pltpu
from jax.sharding import Mesh, PartitionSpec as P

D = 7168
QL = 1536
DL = 512
DR = 64
DC = DL + DR
CTX = 4096
NX, NZ, NY, NC = 4, 8, 4, 2
DP = ("x", "z")
TP = ("y", "c")
CHUNK = 1024
PAD = 64
REL = (0, 3, 1, 2)

epsilon = 1e-06
score_scale = 192.0 ** (-0.5)
masked_score = -1e30


def row_norm(values, gain_vector):
    inverse_rms = lax.rsqrt(jnp.mean(values * values, axis=-1, keepdims=True) + epsilon)
    return values * inverse_rms * gain_vector


def share(block, axes, count):
    copies = jnp.broadcast_to(block[None], (count,) + block.shape)
    return lax.all_to_all(copies, axes, split_axis=0, concat_axis=0, tiled=True)


def swap_cores(block):
    return lax.ppermute(block, "c", [(0, 1), (1, 0)])


def shift(block, axis, step):
    return lax.ppermute(block, axis, [(i, (i + step) % 4) for i in range(4)])


def ring(block, axis):
    half = block.shape[0] // 2
    before = shift(block, axis, 1)
    after = shift(block, axis, -1)
    return block, before, after, shift(before[:half], axis, 1), shift(after[half:], axis, -1)


def attend_kernel(length_ref, xt_ref, fresh_ref, kt_hbm, out_ref, kbuf, sbuf, qbuf, sems):
    slots, rows, _ = out_ref.shape
    chunks = CTX // CHUNK
    row_count, packed, sources = xt_ref.shape
    heads = slots * rows // row_count
    width = packed // heads

    def copy(slot, chunk):
        start = chunk * CHUNK
        if not isinstance(start, int):
            start = pl.multiple_of(start, CHUNK)
        return pltpu.make_async_copy(
            kt_hbm.at[slot, :, pl.ds(start, CHUNK)], kbuf.at[slot, chunk], sems.at[slot, chunk]
        )

    for slot in range(slots):
        for chunk in range(chunks):

            @pl.when(chunk * CHUNK < length_ref[slot])
            def _():
                copy(slot, chunk).start()

    pieces = [
        xt_ref[:, w * heads : (w + 1) * heads, :].reshape(slots * rows, sources)
        for w in range(width)
    ]
    source = lax.broadcasted_iota(jnp.int32, (DC, DC), 0)
    target = lax.broadcasted_iota(jnp.int32, (DC, DC), 1)
    order = target == (source % sources) * width + source // sources
    order = jnp.where(order, 1.0, 0.0).astype(jnp.bfloat16)
    q_all = jnp.dot(
        jnp.concatenate(pieces, axis=1), order, preferred_element_type=jnp.float32
    ).astype(jnp.bfloat16)
    qbuf[...] = q_all.reshape(slots, rows, DC)

    def one_slot(slot, carry):
        length = length_ref[slot]
        live = (length + (CHUNK - 1)) // CHUNK
        q = qbuf[slot]
        fresh = fresh_ref[slot]
        new = lax.dot_general(q, fresh, (((1,), (1,)), ((), ())), preferred_element_type=jnp.float32)
        new = new * score_scale
        key_at = lax.broadcasted_iota(jnp.int32, new.shape, 1)
        step_at = lax.broadcasted_iota(jnp.int32, new.shape, 0) // (rows // 2)
        new = jnp.where(key_at <= step_at, new, masked_score)

        def straight(count):
            peak = jnp.max(new, axis=-1, keepdims=True)
            wide = jnp.full((rows, 128), masked_score, jnp.float32)
            for chunk in range(count):
                copy(slot, chunk).wait()
                s = jnp.dot(q, kbuf[slot, chunk], preferred_element_type=jnp.float32) * score_scale
                if chunk == count - 1:
                    at = chunk * CHUNK + lax.broadcasted_iota(jnp.int32, s.shape, 1)
                    s = jnp.where(at < length, s, masked_score)
                sbuf[chunk] = s
                for lane in range(0, CHUNK, 128):
                    wide = jnp.maximum(wide, s[:, lane : lane + 128])
            peak = jnp.maximum(peak, jnp.max(wide, axis=-1, keepdims=True))
            lifted = jnp.exp(new - peak)
            wide = jnp.zeros((rows, 128), jnp.float32)
            for chunk in range(count):
                e = jnp.exp(sbuf[chunk] - peak)
                sbuf[chunk] = e
                for lane in range(0, CHUNK, 128):
                    wide = wide + e[:, lane : lane + 128]
            total = jnp.sum(wide, axis=-1, keepdims=True)
            total = total + jnp.sum(lifted, axis=-1, keepdims=True)
            inverse = 1.0 / total
            mixed = jnp.dot(
                (lifted * inverse).astype(jnp.bfloat16),
                fresh[:, :DL],
                preferred_element_type=jnp.float32,
            )
            for chunk in range(count):
                weight = (sbuf[chunk] * inverse).astype(jnp.bfloat16)
                mixed = mixed + lax.dot_general(
                    weight,
                    kbuf[slot, chunk, :DL, :],
                    (((1,), (1,)), ((), ())),
                    preferred_element_type=jnp.float32,
                )
            out_ref[slot] = mixed.astype(jnp.bfloat16)

        for count in range(1, chunks + 1):
            pl.when(live == count)(lambda count=count: straight(count))
        return carry

    lax.fori_loop(0, slots, one_slot, 0)


def attend(lengths, packed, fresh, cache):
    slots = cache.shape[0]
    rows = packed.shape[0] * (packed.shape[1] * packed.shape[2] // DC) // slots
    keys = jnp.swapaxes(cache, 1, 2)
    return pl.pallas_call(
        attend_kernel,
        out_shape=jax.ShapeDtypeStruct((slots, rows, DL), jnp.bfloat16),
        grid_spec=pltpu.PrefetchScalarGridSpec(
            num_scalar_prefetch=1,
            grid=(1,),
            in_specs=[
                pl.BlockSpec(packed.shape, lambda i, n: (0, 0, 0)),
                pl.BlockSpec(fresh.shape, lambda i, n: (0, 0, 0)),
                pl.BlockSpec(memory_space=pl.ANY),
            ],
            out_specs=pl.BlockSpec((slots, rows, DL), lambda i, n: (0, 0, 0)),
            scratch_shapes=[
                pltpu.VMEM((slots, CTX // CHUNK, DC, CHUNK), jnp.bfloat16),
                pltpu.VMEM((CTX // CHUNK, rows, CHUNK), jnp.float32),
                pltpu.VMEM((slots, rows, DC), jnp.bfloat16),
                pltpu.SemaphoreType.DMA((slots, CTX // CHUNK)),
            ],
        ),
        compiler_params=pltpu.CompilerParams(vmem_limit_bytes=46 * 1024 * 1024),
        name="attend",
    )(lengths, packed, fresh, keys)


HALF = D // (NX * NZ * NC)


PIECES = 5


def piece_of(refs, k, m, group):
    outer, inner = (m, k) if group == 0 else (k, m)
    refs = refs[group * PIECES : (group + 1) * PIECES]
    if outer < 3:
        return refs[outer], inner
    if inner < 2:
        return refs[3], inner
    return refs[4], inner - 2


def head_kernel(place_ref, gain_ref, weight_hbm, other_hbm, *rest):
    refs, rest = rest[: 2 * PIECES], rest[2 * PIECES :]
    out_ref, wbuf, abuf, bbuf, nbuf, wsem, sem = rest
    x0, y0, core = place_ref[0], place_ref[1], place_ref[2]
    bufs = abuf, bbuf

    def block_copy(group, k, m):
        ref, at = piece_of(refs, k, m, group)
        return pltpu.make_async_copy(ref.at[at], bufs[group].at[k, m], sem.at[group, k, m])

    def weight_copies(k):
        at = (x0 + REL[k]) % NX
        return (
            pltpu.make_async_copy(weight_hbm.at[at, :, core], wbuf.at[k, 0], wsem.at[k, 0]),
            pltpu.make_async_copy(other_hbm.at[at], wbuf.at[k, 1], wsem.at[k, 1]),
        )

    for k in range(NX):
        for m in range(NY):
            block_copy(0, k, m).start()
    for k in range(NX):
        for m in range(NY):
            block_copy(1, k, m).start()
        for copy in weight_copies(k):
            copy.start()
    for k in range(NX):
        for m in range(NY):
            block_copy(0, k, m).wait()
    inverse = []
    for m in range(NY):
        total = jnp.zeros((16, 128), jnp.float32)
        for k in range(NX):
            total = total + abuf[k, m, NZ // 2 * HALF :, :].astype(jnp.float32)
        inverse.append(lax.rsqrt(jnp.sum(total, axis=0, keepdims=True) / D + epsilon))
    for k in range(NX):
        gain = jnp.transpose(gain_ref[(x0 + REL[k]) % NX, core])
        for m in range(NY):
            block_copy(1, k, m).wait()
        for z in range(NZ):
            column = gain[:, z : z + 1]
            at = z % (NZ // 2) * HALF
            for m in range(NY):
                v = bufs[z // (NZ // 2)][k, m, at : at + HALF, :].astype(jnp.float32)
                nbuf[k % 2, m, z] = (v * inverse[m] * column).astype(jnp.bfloat16)
        for copy in weight_copies(k):
            copy.wait()
        for part in range(NC):
            weight = wbuf[k, part].reshape(NZ * HALF, wbuf.shape[-1])
            for m in range(NY):
                term = lax.dot_general(
                    nbuf[k % 2, m].reshape(NZ * HALF, 128),
                    weight,
                    (((0,), (0,)), ((), ())),
                    preferred_element_type=jnp.float32,
                )
                at = (y0 + REL[m]) % NY
                if k == 0:
                    out_ref[part, at] = term
                else:
                    out_ref[part, at] += term


def head(place, gain, weight, other, pieces):
    width = weight.shape[-1]
    vmem = pl.BlockSpec(memory_space=pltpu.VMEM)
    far = pl.BlockSpec(memory_space=pltpu.HBM)
    gain = jnp.transpose(gain.reshape(NX, NZ, NC, HALF), (0, 2, 1, 3))
    return pl.pallas_call(
        head_kernel,
        out_shape=jax.ShapeDtypeStruct((NC, NY, 128, width), jnp.float32),
        in_specs=[pl.BlockSpec(memory_space=pltpu.SMEM), vmem, far, far] + [far] * len(pieces),
        out_specs=vmem,
        scratch_shapes=[
            pltpu.VMEM((NX, NC, NZ, HALF, width), jnp.bfloat16),
            pltpu.VMEM((NX, NY) + pieces[0].shape[1:], jnp.bfloat16),
            pltpu.VMEM((NX, NY) + pieces[PIECES].shape[1:], jnp.bfloat16),
            pltpu.VMEM((2, NY, NZ, HALF, 128), jnp.bfloat16),
            pltpu.SemaphoreType.DMA((NX, NC)),
            pltpu.SemaphoreType.DMA((2, NX, NY)),
        ],
        compiler_params=pltpu.CompilerParams(vmem_limit_bytes=60 * 1024 * 1024),
        name="head",
    )(place, gain, weight, other, *pieces)


def project_kernel(
    owner_ref, mine_ref, rows_ref, other_ref, weight_ref, stream_ref, out_ref, fresh_ref
):
    half = rows_ref.shape[0]
    count = half * NC
    width = weight_ref.shape[0]
    total = None
    fresh = None
    requests = owner_ref.shape[1]
    owner = jnp.broadcast_to(owner_ref[...].astype(jnp.float32), (8, requests))
    owner = owner.astype(jnp.bfloat16)
    place = lax.broadcasted_iota(jnp.int32, (1, half), 1)
    base = ((place >> 6) * NZ + ((place >> 1) & (NZ - 1))) * (NY * NC) + ((place >> 4) & 3) * NC
    for part, ref in enumerate((rows_ref, other_ref)):
        term = lax.dot_general(
            ref[:, :QL], weight_ref[...], (((1,), (1,)), ((), ())),
            preferred_element_type=jnp.float32,
        ).astype(jnp.bfloat16)
        core = mine_ref[2] if part == 0 else 1 - mine_ref[2]
        holds = lax.broadcasted_iota(jnp.int32, (requests, half), 0) == base + core
        holds = jnp.where(holds, 1.0, 0.0).astype(jnp.bfloat16)
        slot = jnp.dot(owner, holds, preferred_element_type=jnp.float32)[:1]
        slot = slot.astype(jnp.int32) * 2 + (place & 1)
        wanted = lax.broadcasted_iota(jnp.int32, (count, half), 0)
        pick = jnp.where(slot == wanted, 1.0, 0.0).astype(jnp.bfloat16)
        term = jnp.dot(pick, term, preferred_element_type=jnp.float32)
        total = term if total is None else total + term
        local = fresh_ref.shape[0]
        wanted = lax.broadcasted_iota(jnp.int32, (local, half), 0) + mine_ref[0]
        pick = jnp.where(slot == wanted, 1.0, 0.0).astype(jnp.bfloat16)
        term = jnp.dot(pick, ref[:, QL : QL + DC], preferred_element_type=jnp.float32)
        fresh = term if fresh is None else fresh + term
    fresh_ref[...] = fresh.astype(jnp.bfloat16)
    out_ref[:, :width] = total.astype(jnp.bfloat16)
    local = fresh_ref.shape[0]
    lane_rows = local // NY
    piece = HALF // NY
    hidden = stream_ref[...].astype(jnp.float32)
    chosen = hidden[:lane_rows]
    for y in range(1, NY):
        chosen = jnp.where(mine_ref[1] == y, hidden[y * lane_rows : (y + 1) * lane_rows], chosen)
    for dest in range(NX * NZ):
        at = dest * NC * HALF
        wide = jnp.where(
            mine_ref[2] == 0, chosen[:, at : at + HALF], chosen[:, at + HALF : at + NC * HALF]
        )
        block = jnp.concatenate([wide[:, q * piece : (q + 1) * piece] for q in range(NY)], axis=0)
        out_ref[dest * local : (dest + 1) * local, width:] = block.astype(jnp.bfloat16)


def project(owner, mine, rows, other, weight, stream):
    count = rows.shape[0] * NC
    local = count // (NX * NZ)
    vmem = pl.BlockSpec(memory_space=pltpu.VMEM)
    return pl.pallas_call(
        project_kernel,
        out_shape=(
            jax.ShapeDtypeStruct((count, weight.shape[0] + HALF // NY), jnp.bfloat16),
            jax.ShapeDtypeStruct((local, DC), jnp.bfloat16),
        ),
        in_specs=[vmem, pl.BlockSpec(memory_space=pltpu.SMEM), vmem, vmem, vmem, vmem],
        out_specs=(vmem, vmem),
        compiler_params=pltpu.CompilerParams(vmem_limit_bytes=32 * 1024 * 1024),
        name="project",
    )(owner.reshape(1, -1), mine, rows, other, weight, stream)


def merge(peak, total, hit):
    top = jnp.max(peak, axis=0)
    return top, jnp.sum(total * jnp.exp(peak - top[None]), axis=0), jnp.sum(hit, axis=0)


def on_device(
    hidden_state,
    attention_gain,
    down_weight,
    query_gain,
    latent_gain,
    query_weight,
    latent_cache,
    cache_length,
    owner_place,
    accept_length,
    value_weight,
    output_weight,
    final_gain,
    head_weight,
    draft_tokens,
):
    x, z, y, c = (lax.axis_index(a) for a in ("x", "z", "y", "c"))
    d = x * NZ + z
    t = y * NC + c
    dp_count, tp_count = NX * NZ, NY * NC
    request_count, step_count = draft_tokens.shape
    row_count = request_count * step_count
    local_requests = latent_cache.shape[0]
    local_rows = local_requests * step_count
    slice_width = query_weight.shape[1]
    local_heads, _, value_width = value_weight.shape
    own_rows = local_rows // tp_count
    step_index = jnp.arange(step_count, dtype=jnp.int32)

    stream = hidden_state.astype(jnp.float32)
    scaled = (stream * attention_gain[:, None]).astype(jnp.bfloat16)
    column_part = lax.dot_general(
        scaled, down_weight, (((0,), (0,)), ((), ())), preferred_element_type=jnp.float32
    )
    inverse_norm = lax.rsqrt(jnp.sum(stream * stream, axis=0) / D + epsilon)
    column_part = column_part * inverse_norm[:, None]
    latent = lax.all_to_all(
        column_part.reshape(tp_count, own_rows, -1), TP, split_axis=0, concat_axis=0, tiled=True
    )
    latent = jnp.swapaxes(latent, 0, 1).reshape(own_rows, QL + DC)
    query_latent = row_norm(latent[:, :QL], query_gain)
    latent_part = row_norm(latent[:, QL : QL + DL], latent_gain)
    blank = jnp.zeros((own_rows, PAD), jnp.float32)
    rows = jnp.concatenate([query_latent, latent_part, latent[:, QL + DL :], blank], axis=1)
    rows = rows.astype(jnp.bfloat16)

    rows = share(rows, "z", NZ).reshape(NZ * own_rows, -1)
    rows = share(rows, ("x", "y"), NX * NY).reshape(row_count // NC, -1)
    other_rows = swap_cores(rows)
    weight = jnp.swapaxes(query_weight, 0, 1).reshape(slice_width * local_heads, QL)
    owner_row = (owner_place[:, None] * step_count + step_index[None, :]).reshape(row_count)
    row_index = jnp.arange(row_count, dtype=jnp.int32)

    lane_rows = local_rows // NY
    width = slice_width * local_heads
    payload, own_fresh = project(
        owner_place,
        jnp.stack([d * local_rows, y, c]),
        rows,
        other_rows,
        weight,
        jnp.swapaxes(hidden_state, 0, 1),
    )
    own_fresh = own_fresh.reshape(local_requests, step_count, DC)
    arrived = lax.all_to_all(
        payload.reshape(dp_count, local_rows, -1), DP, split_axis=0, concat_axis=0, tiled=True
    )
    stream_block = arrived[:, :, width:].reshape(dp_count, NY, lane_rows, HALF // NY)
    stream_block = jnp.transpose(stream_block, (1, 3, 0, 2)).reshape(HALF, dp_count * lane_rows)
    packed = jnp.transpose(arrived[:, :, :width], (1, 2, 0))

    fresh_padded = jnp.pad(own_fresh, ((0, 0), (0, 16 - step_count), (0, 0)))
    attended = attend(cache_length, packed, fresh_padded, latent_cache)
    attended = attended.reshape(local_requests, step_count, local_heads, DL)
    head_values = jnp.einsum(
        "ushc,hcv->ushv", attended, value_weight, preferred_element_type=jnp.float32
    )
    head_values = head_values.astype(jnp.bfloat16).reshape(local_rows, local_heads * value_width)
    head_values = share(head_values, "z", NZ).reshape(NZ * local_rows, -1)
    head_values = jnp.concatenate(ring(head_values, "x"))

    turned = row_index.reshape(dp_count, NY, lane_rows).swapaxes(0, 1).reshape(row_count)
    turned_owner = owner_row.reshape(dp_count, NY, lane_rows).swapaxes(0, 1).reshape(row_count)
    relative = row_index // (NZ * local_rows)
    relative = jnp.where(relative == 1, 3, jnp.where(relative == 0, 0, relative - 1))
    held = (x + relative) % NX * (NZ * local_rows)
    held = held + row_index % (NZ * local_rows)
    turn = (turned_owner[:, None] == held[None, :]).astype(jnp.bfloat16)
    head_values = jnp.dot(turn, head_values, preferred_element_type=jnp.float32)
    head_values = head_values.astype(jnp.bfloat16)
    terms = lax.dot_general(
        output_weight, head_values, (((1,), (1,)), ((), ())), preferred_element_type=jnp.float32
    )
    terms = terms.reshape(NC, HALF, row_count)
    kept = lax.dynamic_index_in_dim(terms, c, 0, keepdims=False)
    sent = lax.dynamic_index_in_dim(terms, 1 - c, 0, keepdims=False)
    kept = kept + swap_cores(sent)
    kept = jnp.swapaxes(kept.reshape(HALF, NY, row_count // NY), 0, 1)
    kept = lax.all_to_all(kept, "y", split_axis=0, concat_axis=0, tiled=True)
    residual = (jnp.sum(kept, axis=0) + stream_block.astype(jnp.float32)).astype(jnp.bfloat16)

    residual = share(residual, "z", NZ)
    squares = residual.astype(jnp.float32)
    squares = jnp.sum(squares * squares, axis=(0, 1))
    squares = squares + swap_cores(squares)
    high = lax.reduce_precision(squares, 8, 7)
    middle = lax.reduce_precision(squares - high, 8, 7)
    parts = jnp.stack([high, middle, squares - high - middle])
    parts = jnp.pad(parts, ((0, 16 - 3), (0, 0))).astype(jnp.bfloat16)
    residual = residual.reshape(NZ * HALF, -1)
    halves = jnp.concatenate([residual[: NZ // 2 * HALF], parts]), residual[NZ // 2 * HALF :]

    def whole(block, axis):
        return jnp.stack([block] + [shift(block, axis, step) for step in (1, -1, 2)])

    pieces = ring(whole(halves[0], "x"), "y") + ring(whole(halves[1], "y"), "x")
    place_of = jnp.stack([x, y, c])
    vocab_width = head_weight.shape[1]
    head_weight = head_weight.reshape(NX, NZ, NC, HALF, vocab_width)
    other = swap_cores(lax.dynamic_index_in_dim(head_weight, 1 - c, 2, keepdims=False))
    logits = head(place_of, final_gain, head_weight, other, pieces)
    logits = logits[0] + swap_cores(logits[1])
    logits = logits.reshape(row_count, vocab_width)
    vocab_start = (d * tp_count + t) * vocab_width

    def turn_rows(flat):
        return flat.reshape(dp_count, NY, lane_rows).swapaxes(0, 1).reshape(row_count)

    target_hit = (turn_rows(draft_tokens) - vocab_start)[:, None] == jnp.arange(
        vocab_width, dtype=jnp.int32
    )[None, :]
    hit = jnp.sum(jnp.where(target_hit, logits, jnp.zeros_like(logits)), axis=1)
    peak = jnp.max(logits, axis=1)
    total = jnp.sum(jnp.exp(logits - peak[:, None]), axis=1)
    stats = jnp.stack([peak, total, hit]).reshape(3, NY, 128)
    stats = jnp.stack([stats, swap_cores(stats)])
    stats = jnp.stack(merge(stats[:, 0], stats[:, 1], stats[:, 2]))
    stats = share(stats, "y", NY)
    stats = jnp.stack(merge(stats[:, 0], stats[:, 1], stats[:, 2]))
    stats = share(stats, DP, dp_count)
    peak, total, target = merge(stats[:, 0], stats[:, 1], stats[:, 2])
    log_total = (peak + jnp.log(total)).reshape(row_count)
    target = target.reshape(row_count)
    accepted = turn_rows((step_index[None, :] < accept_length[:, None]).reshape(row_count))
    log_probs = jnp.where(accepted[:, None], logits - log_total[:, None], jnp.zeros_like(logits))
    draft_scores = jnp.where(accepted, target - log_total, jnp.zeros_like(target))

    def back(turned_rows):
        shape = turned_rows.shape[1:]
        turned_rows = turned_rows.reshape((NY, dp_count, lane_rows) + shape)
        return jnp.swapaxes(turned_rows, 0, 1).reshape((row_count,) + shape)

    slot_global = d * local_requests + jnp.arange(local_requests, dtype=jnp.int32)
    slot_match = owner_place[None, :] == slot_global[:, None]
    slot_accept = jnp.sum(
        jnp.where(slot_match, accept_length[None, :], jnp.zeros_like(slot_match, dtype=jnp.int32)),
        axis=1,
    )
    keep_mask = step_index[None, :, None] < slot_accept[:, None, None]
    committed = jnp.where(keep_mask, own_fresh, jnp.zeros_like(own_fresh))
    return (back(log_probs), back(draft_scores), committed)


def solution(mesh):
    split = Mesh(mesh.devices.reshape(NX, NZ, NY, NC), ("x", "z", "y", "c"))
    return jax.shard_map(
        on_device,
        mesh=split,
        in_specs=(
            P(None, DP),
            P(),
            P(None, TP),
            P(),
            P(),
            P(TP, DP, None),
            P(DP, None, None),
            P(DP),
            P(),
            P(),
            P(TP, None, None),
            P(DP, TP),
            P(),
            P(None, DP + TP),
            P(),
        ),
        out_specs=(P(None, DP + TP), P(), P(DP, None, None)),
        check_vma=False,
    )
```

```python
import jax
import jax.numpy as jnp
from jax import lax
from jax.experimental import pallas as pl
from jax.experimental.pallas import tpu as pltpu
from jax.sharding import Mesh, PartitionSpec as P

D = 7168
QL = 1536
DL = 512
DR = 64
DC = DL + DR
CTX = 4096
NX, NZ, NY, NC = 4, 8, 4, 2
DP = ("x", "z")
TP = ("y", "c")
CHUNK = 1024
PAD = 64
REL = (0, 3, 1, 2)

epsilon = 1e-06
score_scale = 192.0 ** (-0.5)
masked_score = -1e30


def row_norm(values, gain_vector):
    inverse_rms = lax.rsqrt(jnp.mean(values * values, axis=-1, keepdims=True) + epsilon)
    return values * inverse_rms * gain_vector


def share(block, axes, count):
    copies = jnp.broadcast_to(block[None], (count,) + block.shape)
    return lax.all_to_all(copies, axes, split_axis=0, concat_axis=0, tiled=True)


def swap_cores(block):
    return lax.ppermute(block, "c", [(0, 1), (1, 0)])


def shift(block, axis, step):
    return lax.ppermute(block, axis, [(i, (i + step) % 4) for i in range(4)])


def ring(block, axis):
    half = block.shape[0] // 2
    before = shift(block, axis, 1)
    after = shift(block, axis, -1)
    return block, before, after, shift(before[:half], axis, 1), shift(after[half:], axis, -1)


def attend_kernel(length_ref, xt_ref, fresh_ref, kt_hbm, out_ref, kbuf, sbuf, qbuf, sems):
    slots, rows, _ = out_ref.shape
    chunks = CTX // CHUNK
    row_count, packed, sources = xt_ref.shape
    heads = slots * rows // row_count
    width = packed // heads

    def copy(slot, chunk):
        start = chunk * CHUNK
        if not isinstance(start, int):
            start = pl.multiple_of(start, CHUNK)
        return pltpu.make_async_copy(
            kt_hbm.at[slot, :, pl.ds(start, CHUNK)], kbuf.at[slot, chunk], sems.at[slot, chunk]
        )

    for slot in range(slots):
        for chunk in range(chunks):

            @pl.when(chunk * CHUNK < length_ref[slot])
            def _():
                copy(slot, chunk).start()

    pieces = [
        xt_ref[:, w * heads : (w + 1) * heads, :].reshape(slots * rows, sources)
        for w in range(width)
    ]
    source = lax.broadcasted_iota(jnp.int32, (DC, DC), 0)
    target = lax.broadcasted_iota(jnp.int32, (DC, DC), 1)
    order = target == (source % sources) * width + source // sources
    order = jnp.where(order, 1.0, 0.0).astype(jnp.bfloat16)
    q_all = jnp.dot(
        jnp.concatenate(pieces, axis=1), order, preferred_element_type=jnp.float32
    ).astype(jnp.bfloat16)
    qbuf[...] = q_all.reshape(slots, rows, DC)

    def one_slot(slot, carry):
        length = length_ref[slot]
        live = (length + (CHUNK - 1)) // CHUNK
        q = qbuf[slot]
        fresh = fresh_ref[slot]
        new = lax.dot_general(q, fresh, (((1,), (1,)), ((), ())), preferred_element_type=jnp.float32)
        new = new * score_scale
        key_at = lax.broadcasted_iota(jnp.int32, new.shape, 1)
        step_at = lax.broadcasted_iota(jnp.int32, new.shape, 0) // (rows // 2)
        new = jnp.where(key_at <= step_at, new, masked_score)

        def straight(count):
            peak = jnp.max(new, axis=-1, keepdims=True)
            wide = jnp.full((rows, 128), masked_score, jnp.float32)
            for chunk in range(count):
                copy(slot, chunk).wait()
                s = jnp.dot(q, kbuf[slot, chunk], preferred_element_type=jnp.float32) * score_scale
                if chunk == count - 1:
                    at = chunk * CHUNK + lax.broadcasted_iota(jnp.int32, s.shape, 1)
                    s = jnp.where(at < length, s, masked_score)
                sbuf[chunk] = s
                for lane in range(0, CHUNK, 128):
                    wide = jnp.maximum(wide, s[:, lane : lane + 128])
            peak = jnp.maximum(peak, jnp.max(wide, axis=-1, keepdims=True))
            lifted = jnp.exp(new - peak)
            wide = jnp.zeros((rows, 128), jnp.float32)
            for chunk in range(count):
                e = jnp.exp(sbuf[chunk] - peak)
                sbuf[chunk] = e
                for lane in range(0, CHUNK, 128):
                    wide = wide + e[:, lane : lane + 128]
            total = jnp.sum(wide, axis=-1, keepdims=True)
            total = total + jnp.sum(lifted, axis=-1, keepdims=True)
            inverse = 1.0 / total
            mixed = jnp.dot(
                (lifted * inverse).astype(jnp.bfloat16),
                fresh[:, :DL],
                preferred_element_type=jnp.float32,
            )
            for chunk in range(count):
                weight = (sbuf[chunk] * inverse).astype(jnp.bfloat16)
                mixed = mixed + lax.dot_general(
                    weight,
                    kbuf[slot, chunk, :DL, :],
                    (((1,), (1,)), ((), ())),
                    preferred_element_type=jnp.float32,
                )
            out_ref[slot] = mixed.astype(jnp.bfloat16)

        for count in range(1, chunks + 1):
            pl.when(live == count)(lambda count=count: straight(count))
        return carry

    lax.fori_loop(0, slots, one_slot, 0)


def attend(lengths, packed, fresh, cache):
    slots = cache.shape[0]
    rows = packed.shape[0] * (packed.shape[1] * packed.shape[2] // DC) // slots
    keys = jnp.swapaxes(cache, 1, 2)
    return pl.pallas_call(
        attend_kernel,
        out_shape=jax.ShapeDtypeStruct((slots, rows, DL), jnp.bfloat16),
        grid_spec=pltpu.PrefetchScalarGridSpec(
            num_scalar_prefetch=1,
            grid=(1,),
            in_specs=[
                pl.BlockSpec(packed.shape, lambda i, n: (0, 0, 0)),
                pl.BlockSpec(fresh.shape, lambda i, n: (0, 0, 0)),
                pl.BlockSpec(memory_space=pl.ANY),
            ],
            out_specs=pl.BlockSpec((slots, rows, DL), lambda i, n: (0, 0, 0)),
            scratch_shapes=[
                pltpu.VMEM((slots, CTX // CHUNK, DC, CHUNK), jnp.bfloat16),
                pltpu.VMEM((CTX // CHUNK, rows, CHUNK), jnp.float32),
                pltpu.VMEM((slots, rows, DC), jnp.bfloat16),
                pltpu.SemaphoreType.DMA((slots, CTX // CHUNK)),
            ],
        ),
        compiler_params=pltpu.CompilerParams(vmem_limit_bytes=46 * 1024 * 1024),
        name="attend",
    )(lengths, packed, fresh, keys)


HALF = D // (NX * NZ * NC)


PIECES = 5


def output_kernel(owner_ref, x_ref, weight_ref, *refs):
    pieces, out_ref = refs[:PIECES], refs[PIECES]
    count = owner_ref.shape[1]
    block = pieces[0].shape[0]
    half = block // 2
    starts = (0, 3 * block, block, 2 * block, 2 * block + half)
    turned = None
    for ref, start in zip(pieces, starts):
        size = ref.shape[0]
        first = (x_ref[0] * block + start) % count
        held = first + lax.broadcasted_iota(jnp.int32, (size, count), 0)
        pick = jnp.where(held == owner_ref[...], 1.0, 0.0).astype(jnp.bfloat16)
        part = lax.dot_general(
            pick, ref[...], (((0,), (0,)), ((), ())), preferred_element_type=jnp.float32
        )
        turned = part if turned is None else turned + part
    out_ref[...] = lax.dot_general(
        weight_ref[...],
        turned.astype(jnp.bfloat16),
        (((1,), (1,)), ((), ())),
        preferred_element_type=jnp.float32,
    )


def output(owner, x, weight, pieces):
    vmem = pl.BlockSpec(memory_space=pltpu.VMEM)
    return pl.pallas_call(
        output_kernel,
        out_shape=jax.ShapeDtypeStruct((weight.shape[0], owner.shape[0]), jnp.float32),
        in_specs=[vmem, pl.BlockSpec(memory_space=pltpu.SMEM)] + [vmem] * (1 + len(pieces)),
        out_specs=vmem,
        compiler_params=pltpu.CompilerParams(vmem_limit_bytes=32 * 1024 * 1024),
        name="output",
    )(owner.reshape(1, -1), x.reshape(1), weight, *pieces)


def piece_of(refs, k, m, group):
    outer, inner = (m, k) if group == 0 else (k, m)
    refs = refs[group * PIECES : (group + 1) * PIECES]
    if outer < 3:
        return refs[outer], inner
    if inner < 2:
        return refs[3], inner
    return refs[4], inner - 2


def head_kernel(place_ref, gain_ref, weight_hbm, other_hbm, *rest):
    refs, rest = rest[: 2 * PIECES], rest[2 * PIECES :]
    out_ref, wbuf, abuf, bbuf, nbuf, wsem, sem = rest
    x0, y0, core = place_ref[0], place_ref[1], place_ref[2]
    bufs = abuf, bbuf

    def block_copy(group, k, m):
        ref, at = piece_of(refs, k, m, group)
        return pltpu.make_async_copy(ref.at[at], bufs[group].at[k, m], sem.at[group, k, m])

    def weight_copies(k):
        at = (x0 + REL[k]) % NX
        return (
            pltpu.make_async_copy(weight_hbm.at[at, :, core], wbuf.at[k, 0], wsem.at[k, 0]),
            pltpu.make_async_copy(other_hbm.at[at], wbuf.at[k, 1], wsem.at[k, 1]),
        )

    for k in range(NX):
        for m in range(NY):
            block_copy(0, k, m).start()
    for k in range(NX):
        for m in range(NY):
            block_copy(1, k, m).start()
        for copy in weight_copies(k):
            copy.start()
    for k in range(NX):
        for m in range(NY):
            block_copy(0, k, m).wait()
    inverse = []
    for m in range(NY):
        total = jnp.zeros((16, 128), jnp.float32)
        for k in range(NX):
            total = total + abuf[k, m, NZ // 2 * HALF :, :].astype(jnp.float32)
        inverse.append(lax.rsqrt(jnp.sum(total, axis=0, keepdims=True) / D + epsilon))
    for k in range(NX):
        gain = jnp.transpose(gain_ref[(x0 + REL[k]) % NX, core])
        for m in range(NY):
            block_copy(1, k, m).wait()
        for z in range(NZ):
            column = gain[:, z : z + 1]
            at = z % (NZ // 2) * HALF
            for m in range(NY):
                v = bufs[z // (NZ // 2)][k, m, at : at + HALF, :].astype(jnp.float32)
                nbuf[k % 2, m, z] = (v * inverse[m] * column).astype(jnp.bfloat16)
        for copy in weight_copies(k):
            copy.wait()
        for part in range(NC):
            weight = wbuf[k, part].reshape(NZ * HALF, wbuf.shape[-1])
            for m in range(NY):
                term = lax.dot_general(
                    nbuf[k % 2, m].reshape(NZ * HALF, 128),
                    weight,
                    (((0,), (0,)), ((), ())),
                    preferred_element_type=jnp.float32,
                )
                at = (y0 + REL[m]) % NY
                if k == 0:
                    out_ref[part, at] = term
                else:
                    out_ref[part, at] += term


def head(place, gain, weight, other, pieces):
    width = weight.shape[-1]
    vmem = pl.BlockSpec(memory_space=pltpu.VMEM)
    far = pl.BlockSpec(memory_space=pltpu.HBM)
    gain = jnp.transpose(gain.reshape(NX, NZ, NC, HALF), (0, 2, 1, 3))
    return pl.pallas_call(
        head_kernel,
        out_shape=jax.ShapeDtypeStruct((NC, NY, 128, width), jnp.float32),
        in_specs=[pl.BlockSpec(memory_space=pltpu.SMEM), vmem, far, far] + [far] * len(pieces),
        out_specs=vmem,
        scratch_shapes=[
            pltpu.VMEM((NX, NC, NZ, HALF, width), jnp.bfloat16),
            pltpu.VMEM((NX, NY) + pieces[0].shape[1:], jnp.bfloat16),
            pltpu.VMEM((NX, NY) + pieces[PIECES].shape[1:], jnp.bfloat16),
            pltpu.VMEM((2, NY, NZ, HALF, 128), jnp.bfloat16),
            pltpu.SemaphoreType.DMA((NX, NC)),
            pltpu.SemaphoreType.DMA((2, NX, NY)),
        ],
        compiler_params=pltpu.CompilerParams(vmem_limit_bytes=60 * 1024 * 1024),
        name="head",
    )(place, gain, weight, other, *pieces)


def project_kernel(
    owner_ref, mine_ref, rows_ref, other_ref, weight_ref, stream_ref, out_ref, fresh_ref
):
    half = rows_ref.shape[0]
    count = half * NC
    width = weight_ref.shape[0]
    total = None
    fresh = None
    requests = owner_ref.shape[1]
    owner = jnp.broadcast_to(owner_ref[...].astype(jnp.float32), (8, requests))
    owner = owner.astype(jnp.bfloat16)
    place = lax.broadcasted_iota(jnp.int32, (1, half), 1)
    base = ((place >> 6) * NZ + ((place >> 1) & (NZ - 1))) * (NY * NC) + ((place >> 4) & 3) * NC
    for part, ref in enumerate((rows_ref, other_ref)):
        term = lax.dot_general(
            ref[:, :QL], weight_ref[...], (((1,), (1,)), ((), ())),
            preferred_element_type=jnp.float32,
        ).astype(jnp.bfloat16)
        core = mine_ref[2] if part == 0 else 1 - mine_ref[2]
        holds = lax.broadcasted_iota(jnp.int32, (requests, half), 0) == base + core
        holds = jnp.where(holds, 1.0, 0.0).astype(jnp.bfloat16)
        slot = jnp.dot(owner, holds, preferred_element_type=jnp.float32)[:1]
        slot = slot.astype(jnp.int32) * 2 + (place & 1)
        wanted = lax.broadcasted_iota(jnp.int32, (count, half), 0)
        pick = jnp.where(slot == wanted, 1.0, 0.0).astype(jnp.bfloat16)
        term = jnp.dot(pick, term, preferred_element_type=jnp.float32)
        total = term if total is None else total + term
        local = fresh_ref.shape[0]
        wanted = lax.broadcasted_iota(jnp.int32, (local, half), 0) + mine_ref[0]
        pick = jnp.where(slot == wanted, 1.0, 0.0).astype(jnp.bfloat16)
        term = jnp.dot(pick, ref[:, QL : QL + DC], preferred_element_type=jnp.float32)
        fresh = term if fresh is None else fresh + term
    fresh_ref[...] = fresh.astype(jnp.bfloat16)
    out_ref[:, :width] = total.astype(jnp.bfloat16)
    local = fresh_ref.shape[0]
    lane_rows = local // NY
    piece = HALF // NY
    hidden = stream_ref[...].astype(jnp.float32)
    chosen = hidden[:lane_rows]
    for y in range(1, NY):
        chosen = jnp.where(mine_ref[1] == y, hidden[y * lane_rows : (y + 1) * lane_rows], chosen)
    for dest in range(NX * NZ):
        at = dest * NC * HALF
        wide = jnp.where(
            mine_ref[2] == 0, chosen[:, at : at + HALF], chosen[:, at + HALF : at + NC * HALF]
        )
        block = jnp.concatenate([wide[:, q * piece : (q + 1) * piece] for q in range(NY)], axis=0)
        out_ref[dest * local : (dest + 1) * local, width:] = block.astype(jnp.bfloat16)


def project(owner, mine, rows, other, weight, stream):
    count = rows.shape[0] * NC
    local = count // (NX * NZ)
    vmem = pl.BlockSpec(memory_space=pltpu.VMEM)
    return pl.pallas_call(
        project_kernel,
        out_shape=(
            jax.ShapeDtypeStruct((count, weight.shape[0] + HALF // NY), jnp.bfloat16),
            jax.ShapeDtypeStruct((local, DC), jnp.bfloat16),
        ),
        in_specs=[vmem, pl.BlockSpec(memory_space=pltpu.SMEM), vmem, vmem, vmem, vmem],
        out_specs=(vmem, vmem),
        compiler_params=pltpu.CompilerParams(vmem_limit_bytes=32 * 1024 * 1024),
        name="project",
    )(owner.reshape(1, -1), mine, rows, other, weight, stream)


def merge(peak, total, hit):
    top = jnp.max(peak, axis=0)
    return top, jnp.sum(total * jnp.exp(peak - top[None]), axis=0), jnp.sum(hit, axis=0)


def on_device(
    hidden_state,
    attention_gain,
    down_weight,
    query_gain,
    latent_gain,
    query_weight,
    latent_cache,
    cache_length,
    owner_place,
    accept_length,
    value_weight,
    output_weight,
    final_gain,
    head_weight,
    draft_tokens,
):
    x, z, y, c = (lax.axis_index(a) for a in ("x", "z", "y", "c"))
    d = x * NZ + z
    t = y * NC + c
    dp_count, tp_count = NX * NZ, NY * NC
    request_count, step_count = draft_tokens.shape
    row_count = request_count * step_count
    local_requests = latent_cache.shape[0]
    local_rows = local_requests * step_count
    slice_width = query_weight.shape[1]
    local_heads, _, value_width = value_weight.shape
    own_rows = local_rows // tp_count
    step_index = jnp.arange(step_count, dtype=jnp.int32)

    stream = hidden_state.astype(jnp.float32)
    scaled = (stream * attention_gain[:, None]).astype(jnp.bfloat16)
    column_part = lax.dot_general(
        scaled, down_weight, (((0,), (0,)), ((), ())), preferred_element_type=jnp.float32
    )
    inverse_norm = lax.rsqrt(jnp.sum(stream * stream, axis=0) / D + epsilon)
    column_part = column_part * inverse_norm[:, None]
    latent = lax.all_to_all(
        column_part.reshape(tp_count, own_rows, -1), TP, split_axis=0, concat_axis=0, tiled=True
    )
    latent = jnp.swapaxes(latent, 0, 1).reshape(own_rows, QL + DC)
    query_latent = row_norm(latent[:, :QL], query_gain)
    latent_part = row_norm(latent[:, QL : QL + DL], latent_gain)
    blank = jnp.zeros((own_rows, PAD), jnp.float32)
    rows = jnp.concatenate([query_latent, latent_part, latent[:, QL + DL :], blank], axis=1)
    rows = rows.astype(jnp.bfloat16)

    rows = share(rows, "z", NZ).reshape(NZ * own_rows, -1)
    rows = share(rows, ("x", "y"), NX * NY).reshape(row_count // NC, -1)
    other_rows = swap_cores(rows)
    weight = jnp.swapaxes(query_weight, 0, 1).reshape(slice_width * local_heads, QL)
    owner_row = (owner_place[:, None] * step_count + step_index[None, :]).reshape(row_count)
    row_index = jnp.arange(row_count, dtype=jnp.int32)

    lane_rows = local_rows // NY
    width = slice_width * local_heads
    payload, own_fresh = project(
        owner_place,
        jnp.stack([d * local_rows, y, c]),
        rows,
        other_rows,
        weight,
        jnp.swapaxes(hidden_state, 0, 1),
    )
    own_fresh = own_fresh.reshape(local_requests, step_count, DC)
    arrived = lax.all_to_all(
        payload.reshape(dp_count, local_rows, -1), DP, split_axis=0, concat_axis=0, tiled=True
    )
    stream_block = arrived[:, :, width:].reshape(dp_count, NY, lane_rows, HALF // NY)
    stream_block = jnp.transpose(stream_block, (1, 3, 0, 2)).reshape(HALF, dp_count * lane_rows)
    packed = jnp.transpose(arrived[:, :, :width], (1, 2, 0))

    fresh_padded = jnp.pad(own_fresh, ((0, 0), (0, 16 - step_count), (0, 0)))
    attended = attend(cache_length, packed, fresh_padded, latent_cache)
    attended = attended.reshape(local_requests, step_count, local_heads, DL)
    head_values = jnp.einsum(
        "ushc,hcv->ushv", attended, value_weight, preferred_element_type=jnp.float32
    )
    head_values = head_values.astype(jnp.bfloat16).reshape(local_rows, local_heads * value_width)
    head_values = share(head_values, "z", NZ).reshape(NZ * local_rows, -1)
    head_pieces = ring(head_values, "x")

    turned = row_index.reshape(dp_count, NY, lane_rows).swapaxes(0, 1).reshape(row_count)
    turned_owner = owner_row.reshape(dp_count, NY, lane_rows).swapaxes(0, 1).reshape(row_count)
    terms = output(turned_owner, x, output_weight, head_pieces)
    terms = terms.reshape(NC, HALF, row_count)
    kept = lax.dynamic_index_in_dim(terms, c, 0, keepdims=False)
    sent = lax.dynamic_index_in_dim(terms, 1 - c, 0, keepdims=False)
    kept = kept + swap_cores(sent)
    kept = jnp.swapaxes(kept.reshape(HALF, NY, row_count // NY), 0, 1)
    kept = lax.all_to_all(kept, "y", split_axis=0, concat_axis=0, tiled=True)
    residual = (jnp.sum(kept, axis=0) + stream_block.astype(jnp.float32)).astype(jnp.bfloat16)

    residual = share(residual, "z", NZ)
    squares = residual.astype(jnp.float32)
    squares = jnp.sum(squares * squares, axis=(0, 1))
    squares = squares + swap_cores(squares)
    high = lax.reduce_precision(squares, 8, 7)
    middle = lax.reduce_precision(squares - high, 8, 7)
    parts = jnp.stack([high, middle, squares - high - middle])
    parts = jnp.pad(parts, ((0, 16 - 3), (0, 0))).astype(jnp.bfloat16)
    residual = residual.reshape(NZ * HALF, -1)
    halves = jnp.concatenate([residual[: NZ // 2 * HALF], parts]), residual[NZ // 2 * HALF :]

    def whole(block, axis):
        return jnp.stack([block] + [shift(block, axis, step) for step in (1, -1, 2)])

    pieces = ring(whole(halves[0], "x"), "y") + ring(whole(halves[1], "y"), "x")
    place_of = jnp.stack([x, y, c])
    vocab_width = head_weight.shape[1]
    head_weight = head_weight.reshape(NX, NZ, NC, HALF, vocab_width)
    other = swap_cores(lax.dynamic_index_in_dim(head_weight, 1 - c, 2, keepdims=False))
    logits = head(place_of, final_gain, head_weight, other, pieces)
    logits = logits[0] + swap_cores(logits[1])
    logits = logits.reshape(row_count, vocab_width)
    vocab_start = (d * tp_count + t) * vocab_width

    def turn_rows(flat):
        return flat.reshape(dp_count, NY, lane_rows).swapaxes(0, 1).reshape(row_count)

    def back(turned_rows):
        shape = turned_rows.shape[1:]
        turned_rows = turned_rows.reshape((NY, dp_count, lane_rows) + shape)
        return jnp.swapaxes(turned_rows, 0, 1).reshape((row_count,) + shape)

    settled = lax.optimization_barrier(back(logits))
    target_hit = (turn_rows(draft_tokens) - vocab_start)[:, None] == jnp.arange(
        vocab_width, dtype=jnp.int32
    )[None, :]
    hit = jnp.sum(jnp.where(target_hit, logits, jnp.zeros_like(logits)), axis=1)
    peak = jnp.max(logits, axis=1)
    total = jnp.sum(jnp.exp(logits - peak[:, None]), axis=1)
    stats = jnp.stack([peak, total, hit]).reshape(3, NY, 128)
    stats = jnp.stack([stats, swap_cores(stats)])
    stats = jnp.stack(merge(stats[:, 0], stats[:, 1], stats[:, 2]))
    stats = share(stats, "y", NY)
    stats = jnp.stack(merge(stats[:, 0], stats[:, 1], stats[:, 2]))
    stats = share(stats, DP, dp_count)
    peak, total, target = merge(stats[:, 0], stats[:, 1], stats[:, 2])
    log_total = back((peak + jnp.log(total)).reshape(row_count))
    target = back(target.reshape(row_count))
    accepted = (step_index[None, :] < accept_length[:, None]).reshape(row_count)
    log_probs = jnp.where(accepted[:, None], settled - log_total[:, None], jnp.zeros_like(logits))
    draft_scores = jnp.where(accepted, target - log_total, jnp.zeros_like(target))

    slot_global = d * local_requests + jnp.arange(local_requests, dtype=jnp.int32)
    slot_match = owner_place[None, :] == slot_global[:, None]
    slot_accept = jnp.sum(
        jnp.where(slot_match, accept_length[None, :], jnp.zeros_like(slot_match, dtype=jnp.int32)),
        axis=1,
    )
    keep_mask = step_index[None, :, None] < slot_accept[:, None, None]
    committed = jnp.where(keep_mask, own_fresh, jnp.zeros_like(own_fresh))
    return (log_probs, draft_scores, committed)


def solution(mesh):
    split = Mesh(mesh.devices.reshape(NX, NZ, NY, NC), ("x", "z", "y", "c"))
    return jax.shard_map(
        on_device,
        mesh=split,
        in_specs=(
            P(None, DP),
            P(),
            P(None, TP),
            P(),
            P(),
            P(TP, DP, None),
            P(DP, None, None),
            P(DP),
            P(),
            P(),
            P(TP, None, None),
            P(DP, TP),
            P(),
            P(None, DP + TP),
            P(),
        ),
        out_specs=(P(None, DP + TP), P(), P(DP, None, None)),
        check_vma=False,
    )
```
